32 devices in a mesh: img: 4 (over y, core), txt: 8 (over z, x).
Axes of the slice: x: 2, y: 2, z: 4, core: 2. Of those that a mesh axis runs over, the one named last changes fastest.
Arguments:
- queries: bfloat16 [1, 5120, 8192], P(None, 'txt', 'img'), may hold values from -128 to 128
- visual_keys: bfloat16 [1, 512, 8192], P(None, 'img'), may hold values from -5 to 5
- visual_values: bfloat16 [1, 512, 8192], P(None, 'img'), may hold values from -6 to 6
- out_grad: bfloat16 [1, 5120, 8192], P(None, 'txt', 'img'), may hold values from -6 to 6
- gate_value: float32 [1, 64], P(None, 'img'), may hold values from -1.5 to 1.5
- image_order: int32 [1, 8], replicated, may hold values from 0 to 7, as said below
- image_seen: int32 [5120], P('txt'), may hold values from 1 to 8
Outputs:
- query_grad: bfloat16 [1, 5120, 8192], P(None, 'txt', 'img')
- key_grad: float32 [1, 512, 8192], P(None, 'txt', 'img')
- value_grad: float32 [1, 512, 8192], P(None, 'txt', 'img')
The draws below stay inside these ranges and needn't reach their ends.
Inputs may be any that keep to these rules, and one draw needn't show every extreme that they name: `image_order`: each row names every image of 0 to 7 once.
All inputs are finite; a program needn't handle non-finite values.
Results may differ from the reference program's by a relative error of at most 0.0058.
Values may be sent and summed in bfloat16 or wider, within the bound.
A program may use at most 128 MiB of HBM per device.

```python
import math
import jax
import jax.numpy as jnp
from jax import lax

D = 8192
H = 64
HD = 128
LAT = 64
IMAGES = 8
LAYERS = 1
TOK_DEV = 640
TOKENS = 5120
KEYS = 512


def order_table(key):
    row_list = [jax.random.permutation(jax.random.fold_in(key, 100 + layer_index), IMAGES) for layer_index in range(LAYERS)]
    return jnp.stack(row_list).astype(jnp.int32)


def key_table(key):
    normal_table = jnp.clip(jax.random.normal(jax.random.fold_in(key, 7), (LAYERS, KEYS, D), jnp.float32), -5.0, 5.0)
    return normal_table


def draw_image_order(key, part):
    return order_table(key)


def draw_visual_keys(key, part):
    return key_table(key).astype(jnp.bfloat16)


def draw_queries(key, part):
    normal_table = jnp.clip(jax.random.normal(jax.random.fold_in(key, 9), (LAYERS, TOKENS, D), jnp.float32), -5.0, 5.0)
    return normal_table.astype(jnp.bfloat16)


def set_ends(drawn, stream_key, low, largest):
    spot = [jax.random.randint(jax.random.fold_in(stream_key, axis), (), 0, length) for axis, length in enumerate(drawn.shape)]
    widest = drawn.shape.index(max(drawn.shape))
    neighbour = spot[:widest] + [(spot[widest] + 1) % drawn.shape[widest]] + spot[widest + 1:]
    return drawn.at[tuple(spot)].set(low).at[tuple(neighbour)].set(largest)


def shard_levels(rng, dims, split, least, largest):
    def one(dim, shards_of):
        heights = jax.random.uniform(jax.random.fold_in(jax.random.fold_in(rng, 6), dim), (shards_of,), jnp.float32, least / len(split), largest / len(split))
        return jnp.repeat(jnp.exp(heights), dims[dim] // shards_of).reshape((-1,) + (1,) * (len(dims) - dim - 1))

    level = one(*split[0])
    for cut in split[1:]:
        level = level * one(*cut)
    return level


def scatter_about(stream_key, extent, width, most, shards=(), dtype=jnp.bfloat16):
    gain = shard_levels(stream_key, extent, shards, -0.22, 0.18) if shards else 1.0
    entries = jax.random.normal(stream_key, extent, jnp.float32) * width * gain
    return jnp.minimum(jnp.maximum(entries, -most), most).astype(dtype)


def setup_inputs(seed: int = 0) -> dict:
    streams_of = jax.random.split(jax.random.key(seed), 8)
    queries = draw_queries(jax.random.fold_in(streams_of[7], 71), 0)
    visual_keys = draw_visual_keys(jax.random.fold_in(streams_of[7], 71), 0)
    visual_values = scatter_about(streams_of[2], (LAYERS, KEYS, D), 1.0, 6.0, ((1, 4),))
    out_grad = scatter_about(streams_of[3], (LAYERS, TOKENS, D), 1.0, 6.0, ((1, 8), (2, 4)))
    gate_value = jnp.clip(jax.random.uniform(streams_of[4], (LAYERS, H), jnp.float32, -1.5, 1.5) * shard_levels(streams_of[4], (LAYERS, H), ((1, 4),), -0.4, 0.0), -1.5, 1.5)
    image_order = draw_image_order(jax.random.fold_in(streams_of[7], 71), 0)
    image_seen = set_ends(jax.random.randint(streams_of[6], (TOKENS,), 1, IMAGES + 1), jax.random.fold_in(streams_of[6], 1), 1, IMAGES).astype(jnp.int32)
    return dict(queries=queries, visual_keys=visual_keys, visual_values=visual_values, out_grad=out_grad, gate_value=gate_value, image_order=image_order, image_seen=image_seen)


def rounded(array):
    return lax.optimization_barrier(array.astype(jnp.bfloat16)).astype(jnp.float32)

def reference(queries, visual_keys, visual_values, out_grad, gate_value, image_order, image_seen):
    score_scale = 1.0 / math.sqrt(HD)
    block_count = TOKENS // TOK_DEV
    query_list = []
    key_list = []
    value_list = []
    for layer_index in range(LAYERS):
        key_image = jnp.broadcast_to(image_order[layer_index][:, None], (IMAGES, LAT)).reshape(KEYS)
        key_heads = visual_keys[layer_index].astype(jnp.float32).reshape(KEYS, H, HD)
        value_heads = visual_values[layer_index].astype(jnp.float32).reshape(KEYS, H, HD)
        factor = jnp.tanh(gate_value[layer_index])

        def block_step(totals, pieces):
            query_block, grad_block, seen_block = pieces
            query_heads = query_block.astype(jnp.float32).reshape(TOK_DEV, H, HD)
            gated_grad = rounded(grad_block.astype(jnp.float32).reshape(TOK_DEV, H, HD) * factor[None, :, None])
            allowed = key_image[None, :] < seen_block[:, None]
            scores = jnp.einsum('thd,khd->htk', query_heads, key_heads) * score_scale
            masked = jnp.where(allowed[None], scores, -1e+30)
            row_max = lax.optimization_barrier(jnp.max(masked, axis=2, keepdims=True))
            exponent = jnp.where(allowed[None], jnp.exp(masked - row_max), 0.0)
            weights = exponent / lax.optimization_barrier(jnp.sum(exponent, axis=2, keepdims=True))
            weight_half = rounded(weights)
            attended = jnp.einsum('htk,khd->thd', weight_half, value_heads)
            row_delta = lax.optimization_barrier(jnp.sum(gated_grad * attended, axis=2))
            weight_grad = jnp.einsum('thd,khd->htk', gated_grad, value_heads)
            score_half = rounded(weights * (weight_grad - jnp.transpose(row_delta)[:, :, None]))
            query_part = (jnp.einsum('htk,khd->thd', score_half, key_heads) * score_scale).astype(jnp.bfloat16)
            key_part = jnp.einsum('htk,thd->khd', score_half, query_heads) * score_scale
            value_part = jnp.einsum('htk,thd->khd', weight_half, gated_grad)
            new_totals = (totals[0] + key_part.reshape(KEYS, D), totals[1] + value_part.reshape(KEYS, D))
            return (new_totals, query_part.reshape(TOK_DEV, D))
        inputs = (queries[layer_index].reshape(block_count, TOK_DEV, D), out_grad[layer_index].reshape(block_count, TOK_DEV, D), image_seen.reshape(block_count, TOK_DEV))
        empty_sum = jnp.zeros((KEYS, D), jnp.float32)
        sums, query_parts = lax.scan(block_step, (empty_sum, empty_sum), inputs)
        query_list.append(query_parts.reshape(TOKENS, D))
        key_list.append(sums[0])
        value_list.append(sums[1])
    return (jnp.stack(query_list), jnp.stack(key_list), jnp.stack(value_list))
```

```python
import functools
import math

import jax
import jax.numpy as jnp
from jax import lax
from jax.experimental import pallas as pl
from jax.experimental.pallas import tpu as pltpu
from jax.sharding import PartitionSpec as P

NT = (((1,), (1,)), ((), ()))
TN = (((0,), (0,)), ((), ()))
NN = (((1,), (0,)), ((), ()))
MESH = pl.DeviceIdType.MESH
LAGS = (2, 4, 6)


def matmul(left, right, dims):
    return lax.dot_general(left, right, dims, preferred_element_type=jnp.float32)


def head_grads(query, gated, key, value, bias):
    rows, tokens = key.shape[0], query.shape[0]
    images = bias.shape[0]
    scale = 1.0 / math.sqrt(query.shape[1])
    scores = matmul(key, query, NT) * (scale * math.log2(math.e))
    masked = (scores.reshape(images, rows // images, tokens) + bias[:, None, :]).reshape(rows, tokens)
    exponent = jnp.exp2(masked - jnp.max(masked, axis=0, keepdims=True))
    weights = exponent * (1.0 / jnp.sum(exponent, axis=0, keepdims=True))
    weight_half = weights.astype(jnp.bfloat16)
    weight_grad = matmul(value, gated, NT)
    delta = jnp.sum(weight_half.astype(jnp.float32) * weight_grad, axis=0, keepdims=True)
    score_half = (weights * (weight_grad - delta)).astype(jnp.bfloat16)
    query_grad = (matmul(key, score_half, TN) * scale).T
    key_grad = matmul(score_half, query, NN) * scale
    value_grad = matmul(weight_half, gated, NN)
    return query_grad, key_grad, value_grad


def kernel(images_n, sides, relief, order_ref, gate_ref, seen_ref, query_ref, grad_ref, key_ref, value_ref,
           out_ref, key_out, value_out,
           bias, queries, grads, latents, full, pair_out, pair_in, edge_out, edge_in, near_out, near_in,
           far_out, far_in,
           load_sem, near_sem, far_sem, latent_send, pair_send, pair_recv, line_send, edge_recv, near_recv,
           far_recv):
    heads = gate_ref.shape[1]
    width = queries.shape[2]
    owned = key_ref.shape[0]
    half = jnp.bfloat16
    pairs = sides // 2
    chips = images_n // 2
    me = lax.axis_index("img")
    place = lax.axis_index("txt")
    mine = place // 2
    side = place % 2
    other = 1 - side
    group = mine // 2
    parity = group % 2
    centre = jnp.where(group < pairs // 2, 1, 0) if pairs > 1 else 1
    inner = mine % 2 == centre
    outer = jnp.logical_not(inner)
    hub = group * 2 + centre
    rim = group * 2 + 1 - centre
    chip = me // 2
    sibling = chip * 2 + 1 - me % 2

    def at(z):
        return {"txt": z * 2 + side}

    def hub_of(g):
        return g * 2 + (jnp.where(g < pairs // 2, 1, 0) if pairs > 1 else 1)

    def columns(index):
        return pl.ds(pl.multiple_of(index * width, width), width)

    def remote(src, dst, send, recv, device):
        return pltpu.make_async_remote_copy(src_ref=src, dst_ref=dst, send_sem=send, recv_sem=recv,
                                            device_id=device, device_id_type=MESH)

    def drain(ref, sem):
        pltpu.make_async_copy(ref, ref, sem).wait()

    def rows_of(owner, count):
        return pl.ds(pl.multiple_of(owner * owned, owned), count * owned)

    takes = jnp.where(inner, parity, 1 - parity)

    def relieved(index):
        return jnp.logical_and(index >= 1, index <= 2 * relief)

    def fetched(index):
        return jnp.logical_or(jnp.logical_not(relieved(index)), (index + 1) % 2 == takes)

    def forwarder(index):
        return jnp.logical_and(inner, jnp.logical_and(relieved(index), fetched(index)))

    def foreign(index, off):
        return latents.at[index, :, rows_of(((chip + off) % chips) * 2, 2), :]

    def forward_copies(index):
        copies = []
        for device in (at(hub_of(group ^ 1)), at(rim)):
            for off in range(1, chips):
                view = foreign(index, off)
                copies.append(remote(view, view, latent_send.at[index], far_sem.at[index], device))
        return copies

    def drain_foreign(index):
        drain(latents.at[index, :, pl.ds(0, (images_n - 2) * owned), :], far_sem.at[index])

    def forward(m):
        index = 1 + 2 * m + parity

        @pl.when(jnp.logical_and(inner, m < relief))
        def _():
            drain_foreign(index)
            for copy in forward_copies(index):
                copy.start()

    def pair_copy(index):
        return remote(pair_out.at[index], pair_in.at[index], pair_send.at[index], pair_recv.at[index],
                      {"txt": mine * 2 + other})

    def edge_copy(index):
        return remote(edge_out.at[index], edge_in.at[index], line_send.at[index], edge_recv.at[index], at(hub))

    def near_copy(index):
        return remote(near_out.at[index], near_in.at[index], line_send.at[index], near_recv.at[index], at(rim))

    def far_copy(index, off, member):
        there = ((group + off) % pairs) * 2 + member
        return remote(far_out.at[index, off - 1, member], far_in.at[index, off - 1],
                      line_send.at[index], far_recv.at[index], at(there))

    barrier = pltpu.get_barrier_semaphore()

    def greet(device):
        pl.semaphore_signal(barrier, inc=1, device_id=device, device_id_type=MESH)

    for off in range(1, images_n):
        greet({"img": (me + off) % images_n})
    greet({"txt": mine * 2 + other})
    greet(at(mine ^ 1))
    for off in range(1, pairs):
        there = (group + off) % pairs
        greet(at(hub_of(there)))

        @pl.when(inner)
        def _():
            greet(at(there * 2 + 1 - (hub_of(there) - there * 2)))

    def load(index):
        return [pltpu.make_async_copy(ref.at[:, columns(index)], buf.at[index], load_sem.at[index])
                for ref, buf in ((query_ref, queries), (grad_ref, grads))]

    for copy in load(0):
        copy.start()
    pl.semaphore_wait(barrier, images_n - 1 + 2 + (pairs - 1) * jnp.where(inner, 2, 1))

    def send(index, carry):
        for slot, ref in enumerate((key_ref, value_ref)):
            target = latents.at[index, slot, rows_of(me, 1), :]
            remote(ref.at[:, columns(sibling * heads + index)], target,
                   latent_send.at[index], near_sem.at[index], {"img": sibling}).start()
            pltpu.make_async_copy(ref.at[:, columns(me * heads + index)], target, near_sem.at[index]).start()

        @pl.when(fetched(index))
        def _():
            for off in range(1, chips):
                for core in range(2):
                    owner = ((chip + off) % chips) * 2 + core
                    for slot, ref in enumerate((key_ref, value_ref)):
                        remote(ref.at[:, columns(owner * heads + index)],
                               latents.at[index, slot, rows_of(me, 1), :],
                               latent_send.at[index], far_sem.at[index], {"img": owner}).start()

        @pl.when(index > 0)
        def _():
            for copy in load(index):
                copy.start()

        return carry

    lax.fori_loop(0, heads, send, 0)
    seen = seen_ref[...].reshape(1, bias.shape[1])
    for i in range(order_ref.shape[1]):
        bias[pl.ds(i, 1), :] = jnp.where(seen > order_ref[0, i], 0.0, -1e30)

    outs = (key_out, value_out)

    def compute(index):
        drain(latents.at[index, :, pl.ds(0, 2 * owned), :], near_sem.at[index])

        @pl.when(index == 1)
        def _():
            forward(0)

        @pl.when(jnp.logical_not(forwarder(index)))
        def _():
            drain_foreign(index)

        @pl.when(jnp.logical_and(index >= 2, index % 2 == 0))
        def _():
            forward(index // 2)

        for copy in load(index):
            copy.wait()
        lane = lax.broadcasted_iota(jnp.int32, gate_ref.shape, 1)
        gate = jnp.sum(jnp.where(lane == index, gate_ref[...], 0.0), axis=1, keepdims=True)
        gated = (grads[index].astype(jnp.float32) * jnp.tanh(gate)).astype(half)
        query_grad, key_grad, value_grad = head_grads(
            queries[index], gated, latents[index, 0], latents[index, 1], bias[...]
        )
        out_ref[:, columns(index)] = query_grad.astype(out_ref.dtype)
        shape = full.shape[2:]
        full[index, 0] = key_grad.reshape(shape)
        full[index, 1] = value_grad.reshape(shape)
        for kind in range(2):
            for z in range(sides):
                pair_out[index, kind, z] = full[index, kind, z * 2 + other].astype(half)
        pair_copy(index).start()

    def line(index, kind, z):
        return full[index, kind, z * 2 + side] + pair_in[index, kind, z].astype(jnp.float32)

    def relay(index):
        pair_copy(index).wait_recv()

        @pl.when(outer)
        def _():
            for j in range(sides - 1):
                for kind in range(2):
                    edge_out[index, j, kind] = line(index, kind, (rim + 1 + j) % sides).astype(half)
            edge_copy(index).start()

        @pl.when(inner)
        def _():
            for kind in range(2):
                near_out[index, kind] = line(index, kind, rim).astype(half)
            near_copy(index).start()

        for kind, out in enumerate(outs):
            out[:, columns(index)] = line(index, kind, mine)

    def merge(index):
        @pl.when(inner)
        def _():
            edge_copy(index).wait_recv()
            for off in range(1, pairs):
                for member in range(2):
                    z = ((group + off) % pairs) * 2 + member
                    for kind in range(2):
                        far_out[index, off - 1, member, kind] = (
                            line(index, kind, z)
                            + edge_in[index, (z - rim - 1 + sides) % sides, kind].astype(jnp.float32)
                        ).astype(half)
                    far_copy(index, off, member).start()
            for kind, out in enumerate(outs):
                out[:, columns(index)] += edge_in[index, (hub - rim - 1 + sides) % sides, kind].astype(jnp.float32)

        @pl.when(outer)
        def _():
            near_copy(index).wait_recv()
            for kind, out in enumerate(outs):
                out[:, columns(index)] += near_in[index, kind].astype(jnp.float32)

    def finish(index):
        drain(far_in.at[index], far_recv.at[index])
        for kind, out in enumerate(outs):
            total = out[:, columns(index)]
            for off in range(1, pairs):
                total = total + far_in[index, off - 1, kind].astype(jnp.float32)
            out[:, columns(index)] = total

    def step(i, carry):
        @pl.when(i < heads)
        def _():
            compute(i)

        stages = [relay, merge] + ([finish] if pairs > 1 else [])
        for lag, stage in zip(LAGS, stages):
            @pl.when(jnp.logical_and(i >= lag, i < heads + lag))
            def _(lag=lag, stage=stage):
                stage(i - lag)

        return carry

    lax.fori_loop(0, heads + LAGS[-1], step, 0)

    def settle(index, carry):
        drain(latents.at[index, :, pl.ds(0, owned), :], latent_send.at[index])

        @pl.when(fetched(index))
        def _():
            drain(latents.at[index, :, pl.ds(0, (images_n - 2) * owned), :], latent_send.at[index])

        @pl.when(forwarder(index))
        def _():
            for copy in forward_copies(index):
                copy.wait_send()

        pair_copy(index).wait_send()

        @pl.when(outer)
        def _():
            edge_copy(index).wait_send()

        @pl.when(inner)
        def _():
            near_copy(index).wait_send()
            for off in range(1, pairs):
                for member in range(2):
                    far_copy(index, off, member).wait_send()

        return carry

    lax.fori_loop(0, heads, settle, 0)


def attention(images_n, texts_n, order, gate, seen, query, grad, key, value):
    tokens, width = query.shape
    heads = gate.shape[1]
    head_width = width // heads
    rows = key.shape[0] * images_n
    sides = texts_n // 2
    pairs = sides // 2
    share = rows // texts_n
    relief = heads // 4 if pairs % 2 == 0 and images_n > 2 else 0
    smem = pl.BlockSpec(memory_space=pltpu.SMEM)
    vmem = pl.BlockSpec(memory_space=pltpu.VMEM)
    hbm = pl.BlockSpec(memory_space=pl.ANY)
    half = jnp.bfloat16
    dma = pltpu.SemaphoreType.DMA((heads,))
    return pl.pallas_call(
        functools.partial(kernel, images_n, sides, relief),
        in_specs=[smem, vmem, vmem, hbm, hbm, hbm, hbm],
        out_specs=[vmem, vmem, vmem],
        out_shape=[pltpu.VMEM((tokens, width), half)] + [pltpu.VMEM((share, width), jnp.float32)] * 2,
        scratch_shapes=[
            pltpu.VMEM((order.shape[1], tokens), jnp.float32),
            pltpu.VMEM((heads, tokens, head_width), half),
            pltpu.VMEM((heads, tokens, head_width), half),
            pltpu.VMEM((heads, 2, rows, head_width), half),
            pltpu.VMEM((heads, 2, texts_n, share, head_width), jnp.float32),
            pltpu.VMEM((heads, 2, sides, share, head_width), half),
            pltpu.VMEM((heads, 2, sides, share, head_width), half),
            pltpu.VMEM((heads, sides - 1, 2, share, head_width), half),
            pltpu.VMEM((heads, sides - 1, 2, share, head_width), half),
            pltpu.VMEM((heads, 2, share, head_width), half),
            pltpu.VMEM((heads, 2, share, head_width), half),
            pltpu.VMEM((heads, max(pairs - 1, 1), 2, 2, share, head_width), half),
            pltpu.VMEM((heads, max(pairs - 1, 1), 2, share, head_width), half),
        ] + [dma] * 10,
        compiler_params=pltpu.CompilerParams(
            vmem_limit_bytes=56 * 1024 * 1024, collective_id=0, has_side_effects=True
        ),
    )(order, gate, seen, query, grad, key, value)


def shards(images_n, texts_n, queries, visual_keys, visual_values, out_grad, gate_value, image_order, image_seen):
    query_grad, key_share, value_share = attention(
        images_n, texts_n, image_order, gate_value, image_seen,
        queries[0], out_grad[0], visual_keys[0], visual_values[0]
    )
    return (query_grad[None], key_share[None], value_share[None])


def solution(mesh):
    placed = (
        P(None, "txt", "img"),
        P(None, "img", None),
        P(None, "img", None),
        P(None, "txt", "img"),
        P(None, "img"),
        P(),
        P("txt"),
    )
    return jax.shard_map(
        functools.partial(shards, mesh.shape["img"], mesh.shape["txt"]),
        mesh=mesh,
        in_specs=placed,
        out_specs=(P(None, "txt", "img"), P(None, "txt", "img"), P(None, "txt", "img")),
        check_vma=False,
    )
```

```python
import functools
import math

import jax
import jax.numpy as jnp
from jax import lax
from jax.experimental import pallas as pl
from jax.experimental.pallas import tpu as pltpu
from jax.sharding import PartitionSpec as P

NT = (((1,), (1,)), ((), ()))
TN = (((0,), (0,)), ((), ()))
NN = (((1,), (0,)), ((), ()))
MESH = pl.DeviceIdType.MESH
LAGS = (2, 4, 6, 9)
RELIEF = 8
DEEP = (7, 11)


def matmul(left, right, dims):
    return lax.dot_general(left, right, dims, preferred_element_type=jnp.float32)


def head_grads(query, gated, key, value, bias):
    rows, tokens = key.shape[0], query.shape[0]
    images = bias.shape[0]
    scale = 1.0 / math.sqrt(query.shape[1])
    scores = matmul(key, query, NT) * (scale * math.log2(math.e))
    masked = (scores.reshape(images, rows // images, tokens) + bias[:, None, :]).reshape(rows, tokens)
    exponent = jnp.exp2(masked - jnp.max(masked, axis=0, keepdims=True))
    weights = exponent * (1.0 / jnp.sum(exponent, axis=0, keepdims=True))
    weight_half = weights.astype(jnp.bfloat16)
    weight_grad = matmul(value, gated, NT)
    delta = jnp.sum(weight_half.astype(jnp.float32) * weight_grad, axis=0, keepdims=True)
    score_half = (weights * (weight_grad - delta)).astype(jnp.bfloat16)
    query_grad = (matmul(key, score_half, TN) * scale).T
    key_grad = matmul(score_half, query, NN) * scale
    value_grad = matmul(weight_half, gated, NN)
    return query_grad, key_grad, value_grad


def kernel(images_n, sides, relief, deep, order_hbm, gate_hbm, seen_hbm, query_ref, grad_ref, key_ref, value_ref,
           out_ref, key_out, value_out,
           order_ref, gate_ref, seen_ref, bias, queries, grads, latents, full, pair_out, pair_in, edge_out, edge_in, near_out, near_in,
           far_out, far_in, deep_edge_out, deep_edge_in, deep_near_out, deep_near_in, deep_far_out, deep_far_in,
           load_sem, near_sem, far_sem, latent_send, pair_send, pair_recv, line_send, edge_recv, near_recv,
           far_recv, own_sem, ready):
    heads = gate_ref.shape[1]
    width = queries.shape[2]
    owned = key_ref.shape[0]
    half = jnp.bfloat16
    wide = jnp.float32
    pairs = sides // 2
    chips = images_n // 2
    me = lax.axis_index("img")
    place = lax.axis_index("txt")
    mine = place // 2
    side = place % 2
    other = 1 - side
    group = mine // 2
    parity = group % 2

    def hub_of(g):
        return g * 2 + (jnp.where(g < pairs // 2, 1, 0) if pairs > 1 else 1)

    hub = hub_of(group)
    rim = group * 4 + 1 - hub
    inner = mine == hub
    outer = mine == rim
    chip = me // 2
    sibling = chip * 2 + 1 - me % 2
    across = {"txt": mine * 2 + other}

    def at(z):
        return {"txt": z * 2 + side}

    def columns(index):
        return pl.ds(pl.multiple_of(index * width, width), width)

    def remote(src, dst, send, recv, device):
        return pltpu.make_async_remote_copy(src_ref=src, dst_ref=dst, send_sem=send, recv_sem=recv,
                                            device_id=device, device_id_type=MESH)

    def drain(ref, sem):
        pltpu.make_async_copy(ref, ref, sem).wait()

    def rows_of(owner, count):
        return pl.ds(pl.multiple_of(owner * owned, owned), count * owned)

    takes = jnp.where(inner, parity, 1 - parity)

    def relieved(index):
        return jnp.logical_and(index >= 1, index <= 2 * relief)

    def fetched(index):
        return jnp.logical_or(jnp.logical_not(relieved(index)), (index + 1) % 2 == takes)

    def forwarder(index):
        return jnp.logical_and(inner, jnp.logical_and(relieved(index), fetched(index)))

    def head_at(i):
        first = 2 * i - 1 + takes
        second = 2 * (i - relief) - takes
        return jnp.where(relieved(i), jnp.where(i <= relief, first, second), i)

    def due(t):
        low = jnp.where(relieved(t), 2 * (t - relief) - 1, t)
        high = jnp.where(relieved(t), jnp.where(t > relief, low + 2, low), t + 1)
        return low, high

    def is_deep(index):
        flag = index < 0
        for b in deep:
            flag = jnp.logical_or(flag, index == b)
        return flag

    def forward_copies(index):
        copies = []
        for device in (at(hub_of(group ^ 1)), at(rim)):
            for off in range(1, chips):
                view = latents.at[index, :, rows_of(((chip + off) % chips) * 2, 2), :]
                copies.append(remote(view, view, latent_send, far_sem.at[index], device))
        return copies

    def pair_copy(index, kind, count=sides):
        view = pl.ds(0, count)
        return remote(pair_out.at[index, kind, view], pair_in.at[index, kind, view],
                      pair_send, pair_recv.at[index, kind], across)

    def edge_copy(index, kind):
        return remote(edge_out.at[index, kind], edge_in.at[index, kind],
                      line_send, edge_recv.at[index, kind], at(hub))

    def near_copy(index, kind):
        return remote(near_out.at[index, kind], near_in.at[index, kind],
                      line_send, near_recv.at[index, kind], at(rim))

    def far_copy(index, kind, off, member):
        return remote(far_out.at[index, kind, off - 1, member], far_in.at[index, kind, off - 1],
                      line_send, far_recv.at[index, kind], at(((group + off) % pairs) * 2 + member))

    def slot(index):
        place = 0
        for n, b in enumerate(deep):
            place = jnp.where(index == b, n, place)
        return place

    def deep_edge_copy(index, kind):
        return remote(deep_edge_out.at[slot(index), kind], deep_edge_in.at[slot(index), kind],
                      line_send, edge_recv.at[index, kind], at(hub))

    def deep_near_copy(index, kind):
        return remote(deep_near_out.at[slot(index), kind], deep_near_in.at[slot(index), kind],
                      line_send, near_recv.at[index, kind], at(rim))

    def deep_far_copy(index, kind, off, member):
        return remote(deep_far_out.at[slot(index), kind, off - 1, member], deep_far_in.at[slot(index), kind, off - 1],
                      line_send, far_recv.at[index, kind], at(((group + off) % pairs) * 2 + member))

    barrier = pltpu.get_barrier_semaphore()

    def greet(device, semaphore=barrier):
        pl.semaphore_signal(semaphore, inc=1, device_id=device, device_id_type=MESH)

    for off in range(1, images_n):
        greet({"img": (me + off) % images_n})
    greet(across)
    greet(at(mine ^ 1))

    @pl.when(inner)
    def _():
        for off in range(1, pairs):
            greet(at(hub_of((group + off) % pairs)))

    small = [pltpu.make_async_copy(ref, buf, own_sem.at[n]) for n, (ref, buf) in enumerate(
        ((order_hbm, order_ref), (gate_hbm, gate_ref), (seen_hbm, seen_ref)))]

    def load(index):
        return [pltpu.make_async_copy(ref.at[:, columns(index)], buf.at[index], load_sem.at[index])
                for ref, buf in ((query_ref, queries), (grad_ref, grads))]

    for copy in small + load(0):
        copy.start()
    pl.semaphore_wait(barrier, images_n + 1 + (pairs - 1) * jnp.where(inner, 1, 0))

    @pl.when(inner)
    def _():
        for off in range(1, pairs):
            greet(at(hub_of((group + off) % pairs)), ready)

    sources = (key_ref, value_ref)

    def latent_copy(index, owner, kind, sem):
        return remote(sources[kind].at[:, columns(owner * heads + index)],
                      latents.at[index, kind, rows_of(me, 1), :],
                      latent_send, sem.at[index], {"img": owner})

    def send(index, carry):
        @pl.when(fetched(index))
        def _():
            for off in range(1, chips):
                for core in range(2):
                    for kind in range(2):
                        latent_copy(index, ((chip + off) % chips) * 2 + core, kind, far_sem).start()

        for kind, ref in enumerate(sources):
            latent_copy(index, sibling, kind, near_sem).start()
            pltpu.make_async_copy(ref.at[:, columns(me * heads + index)],
                                  latents.at[index, kind, rows_of(me, 1), :], near_sem.at[index]).start()

        @pl.when(index > 0)
        def _():
            for copy in load(index):
                copy.start()

        return carry

    lax.fori_loop(0, heads, send, 0)
    for copy in small:
        copy.wait()
    seen = seen_ref[...].reshape(1, bias.shape[1])
    for i in range(order_ref.shape[1]):
        bias[pl.ds(i, 1), :] = jnp.where(seen > order_ref[0, i], 0.0, -1e30)

    outs = (key_out, value_out)
    far_rows = pl.ds(0, (images_n - 2) * owned)

    def compute(index):
        drain(latents.at[index, :, pl.ds(0, 2 * owned), :], near_sem.at[index])
        drain(latents.at[index, :, far_rows, :], far_sem.at[index])

        @pl.when(forwarder(index))
        def _():
            for copy in forward_copies(index):
                copy.start()

        for copy in load(index):
            copy.wait()
        lane = lax.broadcasted_iota(jnp.int32, gate_ref.shape, 1)
        gate = jnp.sum(jnp.where(lane == index, gate_ref[...], 0.0), axis=1, keepdims=True)
        gated = (grads[index].astype(wide) * jnp.tanh(gate)).astype(half)
        query_grad, key_grad, value_grad = head_grads(
            queries[index], gated, latents[index, 0], latents[index, 1], bias[...]
        )
        out_ref[:, columns(index)] = query_grad.astype(out_ref.dtype)
        shape = full.shape[2:]
        full[index, 0] = key_grad.reshape(shape)
        full[index, 1] = value_grad.reshape(shape)

        @pl.when(jnp.logical_not(is_deep(index)))
        def _():
            for kind in (1, 0):
                for z in range(sides):
                    pair_out[index, kind, z] = full[index, kind, z * 2 + other].astype(half)
                pair_copy(index, kind).start()

        @pl.when(is_deep(index))
        def _():
            for kind in (1, 0):
                @pl.when(outer)
                def _():
                    for j in range(sides - 1):
                        for x in range(2):
                            deep_edge_out[slot(index), kind, j, x] = (
                                full[index, kind, ((rim + 1 + j) % sides) * 2 + x].astype(half)
                            )
                    deep_edge_copy(index, kind).start()

                @pl.when(inner)
                def _():
                    for x in range(2):
                        deep_near_out[slot(index), kind, x] = full[index, kind, rim * 2 + x].astype(half)
                    deep_near_copy(index, kind).start()

    def line(index, kind, z):
        return full[index, kind, z * 2 + side] + pair_in[index, kind, z].astype(wide)

    def relay(index, kind):
        pair_copy(index, kind).wait_recv()

        @pl.when(outer)
        def _():
            for j in range(sides - 1):
                edge_out[index, kind, j] = line(index, kind, (rim + 1 + j) % sides).astype(half)
            edge_copy(index, kind).start()

        @pl.when(inner)
        def _():
            near_out[index, kind] = line(index, kind, rim).astype(half)
            near_copy(index, kind).start()

        outs[kind][:, columns(index)] = line(index, kind, mine)

    mid = (hub - rim - 1 + sides) % sides

    def merge(index, kind):
        @pl.when(inner)
        def _():
            edge_copy(index, kind).wait_recv()
            for off in range(1, pairs):
                for member in range(2):
                    z = ((group + off) % pairs) * 2 + member
                    far_out[index, kind, off - 1, member] = (
                        line(index, kind, z) + edge_in[index, kind, (z - rim - 1 + sides) % sides].astype(wide)
                    ).astype(half)
                    far_copy(index, kind, off, member).start()
            outs[kind][:, columns(index)] += edge_in[index, kind, mid].astype(wide)

        @pl.when(outer)
        def _():
            near_copy(index, kind).wait_recv()
            outs[kind][:, columns(index)] += near_in[index, kind].astype(wide)

    def finish(index, kind):
        drain(far_in.at[index, kind], far_recv.at[index, kind])
        total = outs[kind][:, columns(index)]
        for off in range(1, pairs):
            total = total + far_in[index, kind, off - 1].astype(wide)
        outs[kind][:, columns(index)] = total

    def deep_merge(index, kind):
        @pl.when(inner)
        def _():
            deep_edge_copy(index, kind).wait_recv()
            for off in range(1, pairs):
                for member in range(2):
                    z = ((group + off) % pairs) * 2 + member
                    for x in range(2):
                        deep_far_out[slot(index), kind, off - 1, member, x] = (
                            full[index, kind, z * 2 + x]
                            + deep_edge_in[slot(index), kind, (z - rim - 1 + sides) % sides, x].astype(wide)
                        ).astype(half)
                    deep_far_copy(index, kind, off, member).start()
            for x in range(2):
                full[index, kind, mine * 2 + x] += deep_edge_in[slot(index), kind, mid, x].astype(wide)

        @pl.when(outer)
        def _():
            deep_near_copy(index, kind).wait_recv()
            for x in range(2):
                full[index, kind, mine * 2 + x] += deep_near_in[slot(index), kind, x].astype(wide)

    def deep_cross(index, kind):
        drain(deep_far_in.at[slot(index), kind], far_recv.at[index, kind])

        def total(x):
            value = full[index, kind, mine * 2 + x]
            for off in range(1, pairs):
                value = value + deep_far_in[slot(index), kind, off - 1, x].astype(wide)
            return value

        pair_out[index, kind, 0] = total(other).astype(half)
        pair_copy(index, kind, 1).start()
        outs[kind][:, columns(index)] = total(side)

    def deep_finish(index, kind):
        pair_copy(index, kind, 1).wait_recv()
        outs[kind][:, columns(index)] += pair_in[index, kind, 0].astype(wide)

    def both(index, plain, deeper):
        if plain is not None:
            @pl.when(jnp.logical_not(is_deep(index)))
            def _():
                for kind in (1, 0):
                    plain(index, kind)

        if deep and deeper is not None:
            @pl.when(is_deep(index))
            def _():
                for kind in (1, 0):
                    deeper(index, kind)

    def natural(t, plain, deeper):
        low, high = due(t)

        def one(index, carry):
            both(index, plain, deeper)
            return carry

        lax.fori_loop(low, high, one, 0)

    def step(i, carry):
        @pl.when(i < heads)
        def _():
            compute(head_at(i))

        @pl.when(i == LAGS[1])
        def _():
            @pl.when(inner)
            def _():
                pl.semaphore_wait(ready, pairs - 1)

        def after(lag, run):
            @pl.when(jnp.logical_and(i >= lag, i < heads + lag))
            def _():
                run(i - lag)

        after(LAGS[0], lambda t: both(head_at(t), relay, None))
        after(LAGS[1], lambda t: natural(t, merge, deep_merge))
        after(LAGS[2], lambda t: natural(t, finish, deep_cross))
        if deep:
            after(LAGS[3], lambda t: natural(t, None, deep_finish))
        return carry

    last = heads + LAGS[2]
    if deep:
        last = max(last, max(deep) + LAGS[3] + 1)
    lax.fori_loop(0, last, step, 0)

    plain = heads - len(deep)
    drain(latents.at[:, :, pl.ds(0, owned), :], latent_send)
    drain(latents.at[pl.ds(0, heads - relief), :, far_rows, :], latent_send)
    drain(pair_out.at[pl.ds(0, plain)], pair_send)
    if deep:
        drain(pair_out.at[pl.ds(0, len(deep)), :, pl.ds(0, 1)], pair_send)

    @pl.when(outer)
    def _():
        drain(edge_out.at[pl.ds(0, plain)], line_send)
        if deep:
            drain(deep_edge_out, line_send)

    @pl.when(inner)
    def _():
        if relief:
            drain(latents.at[pl.ds(0, 2 * relief), :, far_rows, :], latent_send)
        for ref in (near_out, far_out):
            drain(ref.at[pl.ds(0, plain)], line_send)
        if deep:
            for ref in (deep_near_out, deep_far_out):
                drain(ref, line_send)


def attention(images_n, texts_n, order, gate, seen, query, grad, key, value):
    tokens, width = query.shape
    heads = gate.shape[1]
    head_width = width // heads
    rows = key.shape[0] * images_n
    sides = texts_n // 2
    pairs = sides // 2
    share = rows // texts_n
    relief = heads // RELIEF if pairs % 2 == 0 and images_n > 2 else 0
    deep = tuple(heads * b // 16 for b in DEEP)
    vmem = pl.BlockSpec(memory_space=pltpu.VMEM)
    hbm = pl.BlockSpec(memory_space=pl.ANY)
    half = jnp.bfloat16
    dma = pltpu.SemaphoreType.DMA((heads,))
    kinds = pltpu.SemaphoreType.DMA((heads, 2))
    single = pltpu.SemaphoreType.DMA(())
    block = (share, head_width)
    units = (heads, 2)
    deeps = (max(len(deep), 1), 2)
    return pl.pallas_call(
        functools.partial(kernel, images_n, sides, relief, deep),
        in_specs=[hbm] * 7,
        out_specs=[vmem, vmem, vmem],
        out_shape=[pltpu.VMEM((tokens, width), half)] + [pltpu.VMEM((share, width), jnp.float32)] * 2,
        scratch_shapes=[
            pltpu.SMEM(order.shape, order.dtype), pltpu.VMEM(gate.shape, gate.dtype), pltpu.VMEM(seen.shape, seen.dtype),
            pltpu.VMEM((order.shape[1], tokens), jnp.float32),
            pltpu.VMEM((heads, tokens, head_width), half),
            pltpu.VMEM((heads, tokens, head_width), half),
            pltpu.VMEM((heads, 2, rows, head_width), half),
            pltpu.VMEM((*units, texts_n, *block), jnp.float32),
            pltpu.VMEM((*units, sides, *block), half),
            pltpu.VMEM((*units, sides, *block), half),
            pltpu.VMEM((*units, sides - 1, *block), half),
            pltpu.VMEM((*units, sides - 1, *block), half),
            pltpu.VMEM((*units, *block), half),
            pltpu.VMEM((*units, *block), half),
            pltpu.VMEM((*units, pairs - 1, 2, *block), half),
            pltpu.VMEM((*units, pairs - 1, *block), half),
            pltpu.VMEM((*deeps, sides - 1, 2, *block), half),
            pltpu.VMEM((*deeps, sides - 1, 2, *block), half),
            pltpu.VMEM((*deeps, 2, *block), half),
            pltpu.VMEM((*deeps, 2, *block), half),
            pltpu.VMEM((*deeps, pairs - 1, 2, 2, *block), half),
            pltpu.VMEM((*deeps, pairs - 1, 2, *block), half),
            dma, dma, dma, single, single, kinds, single, kinds, kinds, kinds,
            pltpu.SemaphoreType.DMA((3,)), pltpu.SemaphoreType.REGULAR,
        ],
        compiler_params=pltpu.CompilerParams(
            vmem_limit_bytes=56 * 1024 * 1024, collective_id=0, has_side_effects=True
        ),
    )(order, gate, seen, query, grad, key, value)


def publish(*arrays):
    def body(*refs):
        count = len(arrays)
        sems = refs[-1]
        copies = [pltpu.make_async_copy(refs[n], refs[count + n], sems.at[n]) for n in range(count)]
        for copy in copies:
            copy.start()
        for copy in copies:
            copy.wait()

    return pl.pallas_call(
        body,
        in_specs=[pl.BlockSpec(memory_space=pltpu.VMEM)] * len(arrays),
        out_specs=[pl.BlockSpec(memory_space=pl.ANY)] * len(arrays),
        out_shape=[jax.ShapeDtypeStruct(array.shape, array.dtype) for array in arrays],
        scratch_shapes=[pltpu.SemaphoreType.DMA((len(arrays),))],
        compiler_params=pltpu.CompilerParams(vmem_limit_bytes=1024 * 1024),
    )(*[pltpu.with_memory_space_constraint(array, pltpu.VMEM) for array in arrays])


def shards(images_n, texts_n, queries, visual_keys, visual_values, out_grad, gate_value, image_order, image_seen):
    query_grad, key_share, value_share = publish(*attention(
        images_n, texts_n, image_order, gate_value, image_seen,
        queries[0], out_grad[0], visual_keys[0], visual_values[0]
    ))
    return (query_grad[None], key_share[None], value_share[None])


def solution(mesh):
    placed = (
        P(None, "txt", "img"),
        P(None, "img", None),
        P(None, "img", None),
        P(None, "txt", "img"),
        P(None, "img"),
        P(),
        P("txt"),
    )
    return jax.shard_map(
        functools.partial(shards, mesh.shape["img"], mesh.shape["txt"]),
        mesh=mesh,
        in_specs=placed,
        out_specs=(P(None, "txt", "img"), P(None, "txt", "img"), P(None, "txt", "img")),
        check_vma=False,
    )
```

```python
import functools
import math

import jax
import jax.numpy as jnp
from jax import lax
from jax.experimental import pallas as pl
from jax.experimental.pallas import tpu as pltpu
from jax.sharding import PartitionSpec as P

NT = (((1,), (1,)), ((), ()))
TN = (((0,), (0,)), ((), ()))
NN = (((1,), (0,)), ((), ()))
MESH = pl.DeviceIdType.MESH
LAGS = (2, 4, 6)
DEEP_LAGS = (2, 4, 7)
RELIEF = 5
DEEP = 8
DIRECT = 1


def matmul(left, right, dims):
    return lax.dot_general(left, right, dims, preferred_element_type=jnp.float32)


def head_grads(query, gated, key, value, bias):
    rows, tokens = key.shape[0], query.shape[0]
    images = bias.shape[0]
    scale = 1.0 / math.sqrt(query.shape[1])
    scores = matmul(key, query, NT) * (scale * math.log2(math.e))
    masked = (scores.reshape(images, rows // images, tokens) + bias[:, None, :]).reshape(rows, tokens)
    exponent = jnp.exp2(masked - jnp.max(masked, axis=0, keepdims=True))
    weights = exponent * (1.0 / jnp.sum(exponent, axis=0, keepdims=True))
    weight_half = weights.astype(jnp.bfloat16)
    weight_grad = matmul(value, gated, NT)
    delta = jnp.sum(weight_half.astype(jnp.float32) * weight_grad, axis=0, keepdims=True)
    score_half = (weights * (weight_grad - delta)).astype(jnp.bfloat16)
    query_grad = (matmul(key, score_half, TN) * scale).T
    key_grad = matmul(score_half, query, NN) * scale
    value_grad = matmul(weight_half, gated, NN)
    return query_grad, key_grad, value_grad


def kernel(images_n, sides, relief, direct, order_hbm, gate_hbm, seen_hbm, query_ref, grad_ref, key_ref, value_ref,
           out_ref, key_out, value_out,
           order_ref, gate_ref, seen_ref, bias, queries, grads, latents, full, pair_out, pair_in, edge_out, edge_in, near_out, near_in,
           far_out, far_in, deep_edge_out, deep_edge_in, deep_near_out, deep_near_in, deep_far_out, deep_far_in,
           cross_out, cross_in, direct_out, direct_in, first,
           load_sem, near_sem, far_sem, latent_send, pair_send, pair_recv, line_send, edge_recv, near_recv,
           far_recv, deep_line, deep_far, deep_cross_recv, direct_recv, own_sem, ready, open_line):
    heads = gate_ref.shape[1]
    width = queries.shape[2]
    owned = key_ref.shape[0]
    half = jnp.bfloat16
    wide = jnp.float32
    pairs = sides // 2
    chips = images_n // 2
    me = lax.axis_index("img")
    place = lax.axis_index("txt")
    mine = place // 2
    side = place % 2
    other = 1 - side
    group = mine // 2
    parity = group % 2

    def hub_of(g):
        return g * 2 + (jnp.where(g < pairs // 2, 1, 0) if pairs > 1 else 1)

    hub = hub_of(group)
    rim = group * 4 + 1 - hub
    inner = mine == hub
    outer = mine == rim
    chip = me // 2
    sibling = chip * 2 + 1 - me % 2
    across = {"txt": mine * 2 + other}

    def at(z):
        return {"txt": z * 2 + side}

    def columns(index):
        return pl.ds(pl.multiple_of(index * width, width), width)

    def remote(src, dst, send, recv, device):
        return pltpu.make_async_remote_copy(src_ref=src, dst_ref=dst, send_sem=send, recv_sem=recv,
                                            device_id=device, device_id_type=MESH)

    def drain(ref, sem):
        pltpu.make_async_copy(ref, ref, sem).wait()

    def rows_of(owner, count):
        return pl.ds(pl.multiple_of(owner * owned, owned), count * owned)

    takes = jnp.where(inner, parity, 1 - parity)

    def relieved(index):
        return jnp.logical_and(index >= 1, index <= 2 * relief)

    def fetched(index):
        return jnp.logical_or(jnp.logical_not(relieved(index)), (index + 1) % 2 == takes)

    def forwarder(index):
        return jnp.logical_and(inner, jnp.logical_and(relieved(index), fetched(index)))

    def head_at(i):
        first = 2 * i - 1 + takes
        second = 2 * (i - relief) - takes
        return jnp.where(relieved(i), jnp.where(i <= relief, first, second), i)

    def due(t):
        low = jnp.where(relieved(t), 2 * (t - relief) - 1, t)
        high = jnp.where(relieved(t), jnp.where(t > relief, low + 2, low), t + 1)
        return low, high

    share = full.shape[3]
    deep = cross_out.shape[2] if DEEP <= share // 8 else 0
    top = pl.ds(0, share - deep)
    bottom = pl.ds(share - deep, deep)

    def forward_copies(index):
        copies = []
        for device in (at(hub_of(group ^ 1)), at(rim)):
            for off in range(1, chips):
                view = latents.at[index, :, rows_of(((chip + off) % chips) * 2, 2), :]
                copies.append(remote(view, view, latent_send, far_sem.at[index], device))
        return copies

    def pair_copy(index, kind):
        return remote(pair_out.at[index, kind], pair_in.at[index, kind],
                      pair_send, pair_recv.at[index, kind], across)

    def cross_copy(index):
        return remote(cross_out.at[index], cross_in.at[index], pair_send, deep_cross_recv.at[index], across)

    def edge_copy(index, kind):
        return remote(edge_out.at[index, kind], edge_in.at[index, kind],
                      line_send, edge_recv.at[index, kind], at(hub))

    def near_copy(index, kind):
        return remote(near_out.at[index, kind], near_in.at[index, kind],
                      line_send, near_recv.at[index, kind], at(rim))

    def far_copy(index, kind, off, member):
        return remote(far_out.at[index, kind, off - 1, member], far_in.at[index, kind, off - 1],
                      line_send, far_recv.at[index, kind], at(((group + off) % pairs) * 2 + member))

    def deep_edge_copy(index):
        return remote(deep_edge_out.at[index], deep_edge_in.at[index], line_send, deep_line.at[index], at(hub))

    def deep_near_copy(index):
        return remote(deep_near_out.at[index], deep_near_in.at[index], line_send, deep_line.at[index], at(rim))

    def deep_far_copy(index, off, member):
        return remote(deep_far_out.at[index, off - 1, member], deep_far_in.at[index, off - 1],
                      line_send, deep_far.at[index], at(((group + off) % pairs) * 2 + member))

    barrier = pltpu.get_barrier_semaphore()

    def greet(device, semaphore=barrier):
        pl.semaphore_signal(semaphore, inc=1, device_id=device, device_id_type=MESH)

    for off in range(1, images_n):
        greet({"img": (me + off) % images_n})
    greet(across)
    greet(at(mine ^ 1))

    @pl.when(inner)
    def _():
        for off in range(1, pairs):
            greet(at(hub_of((group + off) % pairs)))

    small = [pltpu.make_async_copy(ref, buf, own_sem.at[n]) for n, (ref, buf) in enumerate(
        ((order_hbm, order_ref), (gate_hbm, gate_ref), (seen_hbm, seen_ref)))]

    def load(index):
        return [pltpu.make_async_copy(ref.at[:, columns(index)], buf.at[index], load_sem.at[index])
                for ref, buf in ((query_ref, queries), (grad_ref, grads))]

    sources = (key_ref, value_ref)
    strangers = [((chip + off) % chips) * 2 + core for off in range(1, chips) for core in range(2)]
    staged = [pltpu.make_async_copy(ref.at[:, columns(owner * heads)], first.at[n, kind], own_sem.at[3])
              for n, owner in enumerate(strangers) for kind, ref in enumerate(sources)]
    for copy in staged + small + load(0):
        copy.start()
    drain(first, own_sem.at[3])
    pl.semaphore_wait(barrier, images_n + 1 + (pairs - 1) * jnp.where(inner, 1, 0))

    @pl.when(inner)
    def _():
        for off in range(1, pairs):
            greet(at(hub_of((group + off) % pairs)), ready)

    def latent_copy(index, owner, kind, sem, source=None):
        source = sources[kind].at[:, columns(owner * heads + index)] if source is None else source
        return remote(source,
                      latents.at[index, kind, rows_of(me, 1), :],
                      latent_send, sem.at[index], {"img": owner})

    def send(index, carry):
        @pl.when(jnp.logical_and(index > 0, fetched(index)))
        def _():
            for owner in strangers:
                for kind in range(2):
                    latent_copy(index, owner, kind, far_sem).start()

        for kind, ref in enumerate(sources):
            latent_copy(index, sibling, kind, near_sem).start()
            pltpu.make_async_copy(ref.at[:, columns(me * heads + index)],
                                  latents.at[index, kind, rows_of(me, 1), :], near_sem.at[index]).start()

        @pl.when(index > 0)
        def _():
            for copy in load(index):
                copy.start()

        return carry

    for n, owner in enumerate(strangers):
        for kind in range(2):
            latent_copy(0, owner, kind, far_sem, first.at[n, kind]).start()
    lax.fori_loop(0, heads, send, 0)
    for copy in small:
        copy.wait()
    seen = seen_ref[...].reshape(1, bias.shape[1])
    for i in range(order_ref.shape[1]):
        bias[pl.ds(i, 1), :] = jnp.where(seen > order_ref[0, i], 0.0, -1e30)

    outs = (key_out, value_out)
    far_rows = pl.ds(0, (images_n - 2) * owned)

    def compute(index):
        drain(latents.at[index, :, pl.ds(0, 2 * owned), :], near_sem.at[index])
        drain(latents.at[index, :, far_rows, :], far_sem.at[index])

        @pl.when(forwarder(index))
        def _():
            for copy in forward_copies(index):
                copy.start()

        for copy in load(index):
            copy.wait()
        lane = lax.broadcasted_iota(jnp.int32, gate_ref.shape, 1)
        gate = jnp.sum(jnp.where(lane == index, gate_ref[...], 0.0), axis=1, keepdims=True)
        gated = (grads[index].astype(wide) * jnp.tanh(gate)).astype(half)
        query_grad, key_grad, value_grad = head_grads(
            queries[index], gated, latents[index, 0], latents[index, 1], bias[...]
        )
        out_ref[:, columns(index)] = query_grad.astype(out_ref.dtype)
        shape = full.shape[2:]
        full[index, 0] = key_grad.reshape(shape)
        full[index, 1] = value_grad.reshape(shape)

        for kind in (1, 0):
            for z in range(sides):
                pair_out[index, kind, z] = full[index, kind, z * 2 + other, top].astype(half)
            pair_copy(index, kind).start()
        if deep:
            @pl.when(outer)
            def _():
                for kind in range(2):
                    for j in range(sides - 1):
                        for x in range(2):
                            deep_edge_out[index, j, x, kind] = (
                                full[index, kind, ((rim + 1 + j) % sides) * 2 + x, bottom].astype(half)
                            )
                deep_edge_copy(index).start()

            @pl.when(inner)
            def _():
                for kind in range(2):
                    for x in range(2):
                        deep_near_out[index, x, kind] = full[index, kind, rim * 2 + x, bottom].astype(half)
                deep_near_copy(index).start()

    def line(index, kind, z):
        return full[index, kind, z * 2 + side, top] + pair_in[index, kind, z].astype(wide)

    def straight(index):
        return index >= heads - direct

    def direct_copy(index, kind, off):
        n = index - (heads - direct)
        return remote(direct_out.at[n, kind, off - 1], direct_in.at[n, kind, off - 1],
                      line_send, direct_recv.at[n, kind], at((mine + off) % sides))

    def relay(index, kind):
        pair_copy(index, kind).wait_recv()
        outs[kind][top, columns(index)] = line(index, kind, mine)

        @pl.when(jnp.logical_not(straight(index)))
        def _():
            relay_plain(index, kind)

        if direct:
            @pl.when(straight(index))
            def _():
                for off in range(1, sides):
                    direct_out[index - (heads - direct), kind, off - 1] = (
                        line(index, kind, (mine + off) % sides).astype(half)
                    )
                    direct_copy(index, kind, off).start()

    def relay_plain(index, kind):
        @pl.when(outer)
        def _():
            for j in range(sides - 1):
                edge_out[index, kind, j] = line(index, kind, (rim + 1 + j) % sides).astype(half)
            edge_copy(index, kind).start()

        @pl.when(inner)
        def _():
            near_out[index, kind] = line(index, kind, rim).astype(half)
            near_copy(index, kind).start()

    mid = (hub - rim - 1 + sides) % sides

    def merge(index, kind):
        @pl.when(jnp.logical_and(inner, jnp.logical_not(straight(index))))
        def _():
            edge_copy(index, kind).wait_recv()
            for off in range(1, pairs):
                for member in range(2):
                    z = ((group + off) % pairs) * 2 + member
                    far_out[index, kind, off - 1, member] = (
                        line(index, kind, z) + edge_in[index, kind, (z - rim - 1 + sides) % sides].astype(wide)
                    ).astype(half)
                    far_copy(index, kind, off, member).start()
            outs[kind][top, columns(index)] += edge_in[index, kind, mid].astype(wide)

        @pl.when(jnp.logical_and(outer, jnp.logical_not(straight(index))))
        def _():
            near_copy(index, kind).wait_recv()
            outs[kind][top, columns(index)] += near_in[index, kind].astype(wide)

    def gather(index, kind, ref, count):
        total = outs[kind][top, columns(index)]
        for n in range(count):
            total = total + ref[n].astype(wide)
        outs[kind][top, columns(index)] = total

    def finish(index, kind):
        @pl.when(jnp.logical_not(straight(index)))
        def _():
            drain(far_in.at[index, kind], far_recv.at[index, kind])
            gather(index, kind, far_in.at[index, kind], pairs - 1)

        if direct:
            @pl.when(straight(index))
            def _():
                n = index - (heads - direct)
                drain(direct_in.at[n, kind], direct_recv.at[n, kind])
                gather(index, kind, direct_in.at[n, kind], sides - 1)

    def deep_merge(index):
        @pl.when(inner)
        def _():
            deep_edge_copy(index).wait_recv()
            for off in range(1, pairs):
                for member in range(2):
                    z = ((group + off) % pairs) * 2 + member
                    for kind in range(2):
                        for x in range(2):
                            deep_far_out[index, off - 1, member, x, kind] = (
                                full[index, kind, z * 2 + x, bottom]
                                + deep_edge_in[index, (z - rim - 1 + sides) % sides, x, kind].astype(wide)
                            ).astype(half)
                    deep_far_copy(index, off, member).start()
            for kind in range(2):
                for x in range(2):
                    full[index, kind, mine * 2 + x, bottom] += deep_edge_in[index, mid, x, kind].astype(wide)

        @pl.when(outer)
        def _():
            deep_near_copy(index).wait_recv()
            for kind in range(2):
                for x in range(2):
                    full[index, kind, mine * 2 + x, bottom] += deep_near_in[index, x, kind].astype(wide)

    def deep_cross(index):
        drain(deep_far_in.at[index], deep_far.at[index])

        def total(kind, x):
            value = full[index, kind, mine * 2 + x, bottom]
            for off in range(1, pairs):
                value = value + deep_far_in[index, off - 1, x, kind].astype(wide)
            return value

        for kind in range(2):
            cross_out[index, kind] = total(kind, other).astype(half)
        cross_copy(index).start()
        for kind in range(2):
            outs[kind][bottom, columns(index)] = total(kind, side)

    def deep_finish(index):
        cross_copy(index).wait_recv()
        for kind in range(2):
            outs[kind][bottom, columns(index)] += cross_in[index, kind].astype(wide)

    def kinds_of(run):
        def each(index):
            for kind in (1, 0):
                run(index, kind)

        return each

    def natural(t, run):
        low, high = due(t)

        def one(index, carry):
            run(index)
            return carry

        lax.fori_loop(low, high, one, 0)

    def step(i, carry):
        @pl.when(i < heads)
        def _():
            compute(head_at(i))

        @pl.when(i == min(LAGS[1], DEEP_LAGS[0]))
        def _():
            @pl.when(inner)
            def _():
                pl.semaphore_wait(ready, pairs - 1)
                if direct:
                    greet(at(rim), open_line)

            if direct:
                @pl.when(outer)
                def _():
                    pl.semaphore_wait(open_line, 1)

        def after(lag, run):
            if lag is None:
                return

            @pl.when(jnp.logical_and(i >= lag, i < heads + lag))
            def _():
                run(i - lag)

        after(DEEP_LAGS[0] if deep else None, lambda t: natural(t, deep_merge))
        after(DEEP_LAGS[1] if deep else None, lambda t: natural(t, deep_cross))
        after(LAGS[1], lambda t: natural(t, kinds_of(merge)))
        after(LAGS[0], lambda t: kinds_of(relay)(head_at(t)))
        after(LAGS[2], lambda t: natural(t, kinds_of(finish)))
        after(DEEP_LAGS[2] if deep else None, lambda t: natural(t, deep_finish))
        return carry

    last = heads + max(LAGS[2], DEEP_LAGS[2] if deep else 0)
    lax.fori_loop(0, last, step, 0)

    drain(latents.at[:, :, pl.ds(0, owned), :], latent_send)
    drain(latents.at[pl.ds(0, heads - relief), :, far_rows, :], latent_send)
    for ref in (pair_out, cross_out) if deep else (pair_out,):
        drain(ref, pair_send)

    plain = pl.ds(0, heads - direct)
    if direct:
        drain(direct_out, line_send)

    @pl.when(outer)
    def _():
        drain(edge_out.at[plain], line_send)
        if deep:
            drain(deep_edge_out, line_send)

    @pl.when(inner)
    def _():
        if relief:
            drain(latents.at[pl.ds(0, 2 * relief), :, far_rows, :], latent_send)
        for ref in (near_out.at[plain], far_out.at[plain]) + ((deep_near_out, deep_far_out) if deep else ()):
            drain(ref, line_send)


def attention(images_n, texts_n, order, gate, seen, query, grad, key, value):
    tokens, width = query.shape
    heads = gate.shape[1]
    head_width = width // heads
    rows = key.shape[0] * images_n
    sides = texts_n // 2
    pairs = sides // 2
    share = rows // texts_n
    relief = heads // RELIEF if pairs % 2 == 0 and images_n > 2 else 0
    deep = DEEP if DEEP <= share // 8 else 0
    vmem = pl.BlockSpec(memory_space=pltpu.VMEM)
    hbm = pl.BlockSpec(memory_space=pl.ANY)
    half = jnp.bfloat16
    dma = pltpu.SemaphoreType.DMA((heads,))
    kinds = pltpu.SemaphoreType.DMA((heads, 2))
    single = pltpu.SemaphoreType.DMA(())
    block = (share - deep, head_width)
    direct = DIRECT if sides <= 4 else 0
    small = (max(deep, 8), head_width)
    units = (heads, 2)
    return pl.pallas_call(
        functools.partial(kernel, images_n, sides, relief, direct),
        in_specs=[hbm] * 7,
        out_specs=[vmem, vmem, vmem],
        out_shape=[pltpu.VMEM((tokens, width), half)] + [pltpu.VMEM((share, width), jnp.float32)] * 2,
        scratch_shapes=[
            pltpu.SMEM(order.shape, order.dtype), pltpu.VMEM(gate.shape, gate.dtype), pltpu.VMEM(seen.shape, seen.dtype),
            pltpu.VMEM((order.shape[1], tokens), jnp.float32),
            pltpu.VMEM((heads, tokens, head_width), half),
            pltpu.VMEM((heads, tokens, head_width), half),
            pltpu.VMEM((heads, 2, rows, head_width), half),
            pltpu.VMEM((*units, texts_n, share, head_width), jnp.float32),
            pltpu.VMEM((*units, sides, *block), half),
            pltpu.VMEM((*units, sides, *block), half),
            pltpu.VMEM((*units, sides - 1, *block), half),
            pltpu.VMEM((*units, sides - 1, *block), half),
            pltpu.VMEM((*units, *block), half),
            pltpu.VMEM((*units, *block), half),
            pltpu.VMEM((*units, pairs - 1, 2, *block), half),
            pltpu.VMEM((*units, pairs - 1, *block), half),
            pltpu.VMEM((heads, sides - 1, 2, 2, *small), half),
            pltpu.VMEM((heads, sides - 1, 2, 2, *small), half),
            pltpu.VMEM((heads, 2, 2, *small), half),
            pltpu.VMEM((heads, 2, 2, *small), half),
            pltpu.VMEM((heads, pairs - 1, 2, 2, 2, *small), half),
            pltpu.VMEM((heads, pairs - 1, 2, 2, *small), half),
            pltpu.VMEM((*units, *small), half),
            pltpu.VMEM((*units, *small), half),
            pltpu.VMEM((max(direct, 1), 2, sides - 1, *block), half),
            pltpu.VMEM((max(direct, 1), 2, sides - 1, *block), half),
            pltpu.VMEM((images_n - 2, 2, rows // images_n, head_width), half),
            dma, dma, dma, single, single, kinds, single, kinds, kinds, kinds,
            dma, dma, dma, pltpu.SemaphoreType.DMA((max(direct, 1), 2)), pltpu.SemaphoreType.DMA((4,)),
            pltpu.SemaphoreType.REGULAR, pltpu.SemaphoreType.REGULAR,
        ],
        compiler_params=pltpu.CompilerParams(
            vmem_limit_bytes=56 * 1024 * 1024, collective_id=0, has_side_effects=True
        ),
    )(order, gate, seen, query, grad, key, value)


def publish(*arrays):
    def body(*refs):
        count = len(arrays)
        sems = refs[-1]
        copies = [pltpu.make_async_copy(refs[n], refs[count + n], sems.at[n]) for n in range(count)]
        for copy in copies:
            copy.start()
        for copy in copies:
            copy.wait()

    return pl.pallas_call(
        body,
        in_specs=[pl.BlockSpec(memory_space=pltpu.VMEM)] * len(arrays),
        out_specs=[pl.BlockSpec(memory_space=pl.ANY)] * len(arrays),
        out_shape=[jax.ShapeDtypeStruct(array.shape, array.dtype) for array in arrays],
        scratch_shapes=[pltpu.SemaphoreType.DMA((len(arrays),))],
        compiler_params=pltpu.CompilerParams(vmem_limit_bytes=1024 * 1024),
    )(*[pltpu.with_memory_space_constraint(array, pltpu.VMEM) for array in arrays])


def shards(images_n, texts_n, queries, visual_keys, visual_values, out_grad, gate_value, image_order, image_seen):
    query_grad, key_share, value_share = publish(*attention(
        images_n, texts_n, image_order, gate_value, image_seen,
        queries[0], out_grad[0], visual_keys[0], visual_values[0]
    ))
    return (query_grad[None], key_share[None], value_share[None])


def solution(mesh):
    placed = (
        P(None, "txt", "img"),
        P(None, "img", None),
        P(None, "img", None),
        P(None, "txt", "img"),
        P(None, "img"),
        P(),
        P("txt"),
    )
    return jax.shard_map(
        functools.partial(shards, mesh.shape["img"], mesh.shape["txt"]),
        mesh=mesh,
        in_specs=placed,
        out_specs=(P(None, "txt", "img"), P(None, "txt", "img"), P(None, "txt", "img")),
        check_vma=False,
    )
```

```python
import functools
import math

import jax
import jax.numpy as jnp
from jax import lax
from jax.experimental import pallas as pl
from jax.experimental.pallas import tpu as pltpu
from jax.sharding import PartitionSpec as P

NT = (((1,), (1,)), ((), ()))
TN = (((0,), (0,)), ((), ()))
NN = (((1,), (0,)), ((), ()))
MESH = pl.DeviceIdType.MESH
LAGS = (2, 4, 6)
DEEP_LAGS = (2, 4, 7)
RELIEF = 5
DEEP = 8
DIRECT = 1


def matmul(left, right, dims):
    return lax.dot_general(left, right, dims, preferred_element_type=jnp.float32)


def head_grads(query, gated, key, value, bias):
    rows, tokens = key.shape[0], query.shape[0]
    images = bias.shape[0]
    scale = 1.0 / math.sqrt(query.shape[1])
    scores = matmul(key, query, NT) * (scale * math.log2(math.e))
    masked = (scores.reshape(images, rows // images, tokens) + bias[:, None, :]).reshape(rows, tokens)
    exponent = jnp.exp2(masked - jnp.max(masked, axis=0, keepdims=True))
    weights = exponent * (1.0 / jnp.sum(exponent, axis=0, keepdims=True))
    weight_half = weights.astype(jnp.bfloat16)
    weight_grad = matmul(value, gated, NT)
    delta = jnp.sum(weight_half.astype(jnp.float32) * weight_grad, axis=0, keepdims=True)
    score_half = (weights * (weight_grad - delta)).astype(jnp.bfloat16)
    query_grad = (matmul(key, score_half, TN) * scale).T
    key_grad = matmul(score_half, query, NN) * scale
    value_grad = matmul(weight_half, gated, NN)
    return query_grad, key_grad, value_grad


def kernel(images_n, sides, relief, direct, order_hbm, gate_hbm, seen_hbm, query_ref, grad_ref, key_ref, value_ref,
           out_ref, key_out, value_out,
           order_ref, gate_ref, seen_ref, bias, queries, grads, latents, full, pair_out, pair_in, edge_out, edge_in, near_out, near_in,
           far_out, far_in, deep_edge_out, deep_edge_in, deep_near_out, deep_near_in, deep_far_out, deep_far_in,
           cross_out, cross_in, direct_out, direct_in, first,
           load_sem, near_sem, far_sem, latent_send, pair_send, pair_recv, line_send, line_recv, last_recv,
           far_recv, deep_line, deep_far, deep_cross_recv, direct_recv, own_sem, ready, open_line):
    heads = gate_ref.shape[1]
    width = queries.shape[2]
    owned = key_ref.shape[0]
    half = jnp.bfloat16
    wide = jnp.float32
    pairs = sides // 2
    chips = images_n // 2
    me = lax.axis_index("img")
    place = lax.axis_index("txt")
    mine = place // 2
    side = place % 2
    other = 1 - side
    group = mine // 2
    parity = group % 2

    def hub_of(g):
        return g * 2 + (jnp.where(g < pairs // 2, 1, 0) if pairs > 1 else 1)

    hub = hub_of(group)
    rim = group * 4 + 1 - hub
    inner = mine == hub
    outer = mine == rim
    chip = me // 2
    sibling = chip * 2 + 1 - me % 2
    across = {"txt": mine * 2 + other}

    def at(z):
        return {"txt": z * 2 + side}

    def columns(index):
        return pl.ds(pl.multiple_of(index * width, width), width)

    def remote(src, dst, send, recv, device):
        return pltpu.make_async_remote_copy(src_ref=src, dst_ref=dst, send_sem=send, recv_sem=recv,
                                            device_id=device, device_id_type=MESH)

    def drain(ref, sem):
        pltpu.make_async_copy(ref, ref, sem).wait()

    def rows_of(owner, count):
        return pl.ds(pl.multiple_of(owner * owned, owned), count * owned)

    takes = jnp.where(inner, parity, 1 - parity)

    def relieved(index):
        return jnp.logical_and(index >= 1, index <= 2 * relief)

    def fetched(index):
        return jnp.logical_or(jnp.logical_not(relieved(index)), (index + 1) % 2 == takes)

    def forwarder(index):
        return jnp.logical_and(inner, jnp.logical_and(relieved(index), fetched(index)))

    def head_at(i):
        first = 2 * i - 1 + takes
        second = 2 * (i - relief) - takes
        return jnp.where(relieved(i), jnp.where(i <= relief, first, second), i)

    def due(t):
        low = jnp.where(relieved(t), 2 * (t - relief) - 1, t)
        high = jnp.where(relieved(t), jnp.where(t > relief, low + 2, low), t + 1)
        return low, high

    share = full.shape[3]
    deep = cross_out.shape[2] if DEEP <= share // 8 else 0
    top = pl.ds(0, share - deep)
    bottom = pl.ds(share - deep, deep)

    def forward_copies(index):
        copies = []
        for device in (at(hub_of(group ^ 1)), at(rim)):
            for off in range(1, chips):
                view = latents.at[index, :, rows_of(((chip + off) % chips) * 2, 2), :]
                copies.append(remote(view, view, latent_send, far_sem.at[index], device))
        return copies

    def pair_copy(index):
        return remote(pair_out.at[index], pair_in.at[index], pair_send, pair_recv.at[index], across)

    def last_copy(index, kind):
        return remote(pair_out.at[index, kind], pair_in.at[index, kind],
                      pair_send, last_recv.at[index - (heads - direct), kind], across)

    def cross_copy(index):
        return remote(cross_out.at[index], cross_in.at[index], pair_send, deep_cross_recv.at[index], across)

    def edge_copy(index):
        return remote(edge_out.at[index], edge_in.at[index], line_send, line_recv.at[index], at(hub))

    def near_copy(index):
        return remote(near_out.at[index], near_in.at[index], line_send, line_recv.at[index], at(rim))

    def far_copy(index, off, member):
        return remote(far_out.at[index, off - 1, member], far_in.at[index, off - 1],
                      line_send, far_recv.at[index], at(((group + off) % pairs) * 2 + member))

    def deep_edge_copy(index):
        return remote(deep_edge_out.at[index], deep_edge_in.at[index], line_send, deep_line.at[index], at(hub))

    def deep_near_copy(index):
        return remote(deep_near_out.at[index], deep_near_in.at[index], line_send, deep_line.at[index], at(rim))

    def deep_far_copy(index, off, member):
        return remote(deep_far_out.at[index, off - 1, member], deep_far_in.at[index, off - 1],
                      line_send, deep_far.at[index], at(((group + off) % pairs) * 2 + member))

    barrier = pltpu.get_barrier_semaphore()

    def greet(device, semaphore=barrier):
        pl.semaphore_signal(semaphore, inc=1, device_id=device, device_id_type=MESH)

    for off in range(1, images_n):
        greet({"img": (me + off) % images_n})
    greet(across)
    greet(at(mine ^ 1))

    @pl.when(inner)
    def _():
        for off in range(1, pairs):
            greet(at(hub_of((group + off) % pairs)))

    small = [pltpu.make_async_copy(ref, buf, own_sem.at[n]) for n, (ref, buf) in enumerate(
        ((order_hbm, order_ref), (gate_hbm, gate_ref), (seen_hbm, seen_ref)))]

    def rest(index):
        return jnp.minimum(index, 1)

    def load(index):
        return [pltpu.make_async_copy(ref.at[:, columns(index)], buf.at[index], load_sem.at[n, rest(index)])
                for n, (ref, buf) in enumerate(((query_ref, queries), (grad_ref, grads)))]

    sources = (key_ref, value_ref)
    strangers = [((chip + off) % chips) * 2 + core for off in range(1, chips) for core in range(2)]
    staged = [pltpu.make_async_copy(ref.at[:, columns(owner * heads)], first.at[n, kind], own_sem.at[3])
              for n, owner in enumerate(strangers) for kind, ref in enumerate(sources)]
    for copy in staged + small + load(0):
        copy.start()
    drain(first, own_sem.at[3])
    pl.semaphore_wait(barrier, images_n + 1 + (pairs - 1) * jnp.where(inner, 1, 0))

    @pl.when(inner)
    def _():
        for off in range(1, pairs):
            greet(at(hub_of((group + off) % pairs)), ready)

    def latent_copy(index, owner, kind, sem, source=None):
        source = sources[kind].at[:, columns(owner * heads + index)] if source is None else source
        return remote(source,
                      latents.at[index, kind, rows_of(me, 1), :],
                      latent_send, sem, {"img": owner})

    def send(index, carry):
        @pl.when(jnp.logical_and(index > 0, fetched(index)))
        def _():
            for owner in strangers:
                for kind in range(2):
                    latent_copy(index, owner, kind, far_sem.at[index]).start()

        for kind, ref in enumerate(sources):
            latent_copy(index, sibling, kind, near_sem.at[rest(index)]).start()
            pltpu.make_async_copy(ref.at[:, columns(me * heads + index)],
                                  latents.at[index, kind, rows_of(me, 1), :], near_sem.at[rest(index)]).start()

        @pl.when(index > 0)
        def _():
            for copy in load(index):
                copy.start()

        return carry

    for n, owner in enumerate(strangers):
        for kind in range(2):
            latent_copy(0, owner, kind, far_sem.at[0], first.at[n, kind]).start()
    lax.fori_loop(0, heads, send, 0)
    for copy in small:
        copy.wait()
    seen = seen_ref[...].reshape(1, bias.shape[1])
    for i in range(order_ref.shape[1]):
        bias[pl.ds(i, 1), :] = jnp.where(seen > order_ref[0, i], 0.0, -1e30)

    outs = (key_out, value_out)
    far_rows = pl.ds(0, (images_n - 2) * owned)

    def arrive(part, count):
        drain(latents.at[pl.ds(0, count), :, pl.ds(0, 2 * owned), :], near_sem.at[part])
        for n, buf in enumerate((queries, grads)):
            drain(buf.at[pl.ds(0, count)], load_sem.at[n, part])

    def compute(i):
        index = head_at(i)

        @pl.when(i == 0)
        def _():
            arrive(0, 1)

        @pl.when(i == 1)
        def _():
            arrive(1, heads - 1)

        drain(latents.at[index, :, far_rows, :], far_sem.at[index])

        @pl.when(forwarder(index))
        def _():
            for copy in forward_copies(index):
                copy.start()

        lane = lax.broadcasted_iota(jnp.int32, gate_ref.shape, 1)
        gate = jnp.sum(jnp.where(lane == index, gate_ref[...], 0.0), axis=1, keepdims=True)
        gated = (grads[index].astype(wide) * jnp.tanh(gate)).astype(half)
        query_grad, key_grad, value_grad = head_grads(
            queries[index], gated, latents[index, 0], latents[index, 1], bias[...]
        )
        out_ref[:, columns(index)] = query_grad.astype(out_ref.dtype)
        shape = full.shape[2:]
        full[index, 0] = key_grad.reshape(shape)
        full[index, 1] = value_grad.reshape(shape)

        for kind in (1, 0):
            for z in range(sides):
                pair_out[index, kind, z] = full[index, kind, z * 2 + other, top].astype(half)
            if direct:
                @pl.when(straight(index))
                def _():
                    last_copy(index, kind).start()

        @pl.when(jnp.logical_not(straight(index)))
        def _():
            pair_copy(index).start()

        if deep:
            @pl.when(outer)
            def _():
                for kind in range(2):
                    for j in range(sides - 1):
                        for x in range(2):
                            deep_edge_out[index, j, x, kind] = (
                                full[index, kind, ((rim + 1 + j) % sides) * 2 + x, bottom].astype(half)
                            )
                deep_edge_copy(index).start()

            @pl.when(inner)
            def _():
                for kind in range(2):
                    for x in range(2):
                        deep_near_out[index, x, kind] = full[index, kind, rim * 2 + x, bottom].astype(half)
                deep_near_copy(index).start()

    def line(index, kind, z):
        return full[index, kind, z * 2 + side, top] + pair_in[index, kind, z].astype(wide)

    def straight(index):
        return index >= heads - direct

    def direct_copy(index, kind, off):
        n = index - (heads - direct)
        return remote(direct_out.at[n, kind, off - 1], direct_in.at[n, kind, off - 1],
                      line_send, direct_recv.at[n, kind], at((mine + off) % sides))

    def relay(index):
        @pl.when(jnp.logical_not(straight(index)))
        def _():
            pair_copy(index).wait_recv()

            @pl.when(outer)
            def _():
                for kind in range(2):
                    for j in range(sides - 1):
                        edge_out[index, kind, j] = line(index, kind, (rim + 1 + j) % sides).astype(half)
                edge_copy(index).start()

            @pl.when(inner)
            def _():
                for kind in range(2):
                    near_out[index, kind] = line(index, kind, rim).astype(half)
                near_copy(index).start()

            for kind in range(2):
                outs[kind][top, columns(index)] = line(index, kind, mine)

        if direct:
            @pl.when(straight(index))
            def _():
                for kind in (1, 0):
                    last_copy(index, kind).wait_recv()
                    for off in range(1, sides):
                        direct_out[index - (heads - direct), kind, off - 1] = (
                            line(index, kind, (mine + off) % sides).astype(half)
                        )
                        direct_copy(index, kind, off).start()
                    outs[kind][top, columns(index)] = line(index, kind, mine)

    mid = (hub - rim - 1 + sides) % sides

    def merge(index):
        @pl.when(jnp.logical_and(inner, jnp.logical_not(straight(index))))
        def _():
            edge_copy(index).wait_recv()
            for off in range(1, pairs):
                for member in range(2):
                    z = ((group + off) % pairs) * 2 + member
                    for kind in range(2):
                        far_out[index, off - 1, member, kind] = (
                            line(index, kind, z) + edge_in[index, kind, (z - rim - 1 + sides) % sides].astype(wide)
                        ).astype(half)
                    far_copy(index, off, member).start()
            for kind in range(2):
                outs[kind][top, columns(index)] += edge_in[index, kind, mid].astype(wide)

        @pl.when(jnp.logical_and(outer, jnp.logical_not(straight(index))))
        def _():
            near_copy(index).wait_recv()
            for kind in range(2):
                outs[kind][top, columns(index)] += near_in[index, kind].astype(wide)

    def gather(index, kind, terms):
        total = outs[kind][top, columns(index)]
        for term in terms:
            total = total + term.astype(wide)
        outs[kind][top, columns(index)] = total

    def finish(index):
        @pl.when(jnp.logical_not(straight(index)))
        def _():
            drain(far_in.at[index], far_recv.at[index])
            for kind in range(2):
                gather(index, kind, [far_in[index, n, kind] for n in range(pairs - 1)])

        if direct:
            @pl.when(straight(index))
            def _():
                n = index - (heads - direct)
                for kind in (1, 0):
                    drain(direct_in.at[n, kind], direct_recv.at[n, kind])
                    gather(index, kind, [direct_in[n, kind, off] for off in range(sides - 1)])

    def deep_merge(index):
        @pl.when(inner)
        def _():
            deep_edge_copy(index).wait_recv()
            for off in range(1, pairs):
                for member in range(2):
                    z = ((group + off) % pairs) * 2 + member
                    for kind in range(2):
                        for x in range(2):
                            deep_far_out[index, off - 1, member, x, kind] = (
                                full[index, kind, z * 2 + x, bottom]
                                + deep_edge_in[index, (z - rim - 1 + sides) % sides, x, kind].astype(wide)
                            ).astype(half)
                    deep_far_copy(index, off, member).start()
            for kind in range(2):
                for x in range(2):
                    full[index, kind, mine * 2 + x, bottom] += deep_edge_in[index, mid, x, kind].astype(wide)

        @pl.when(outer)
        def _():
            deep_near_copy(index).wait_recv()
            for kind in range(2):
                for x in range(2):
                    full[index, kind, mine * 2 + x, bottom] += deep_near_in[index, x, kind].astype(wide)

    def deep_cross(index):
        drain(deep_far_in.at[index], deep_far.at[index])

        def total(kind, x):
            value = full[index, kind, mine * 2 + x, bottom]
            for off in range(1, pairs):
                value = value + deep_far_in[index, off - 1, x, kind].astype(wide)
            return value

        for kind in range(2):
            cross_out[index, kind] = total(kind, other).astype(half)
        cross_copy(index).start()
        for kind in range(2):
            outs[kind][bottom, columns(index)] = total(kind, side)

    def deep_finish(index):
        cross_copy(index).wait_recv()
        for kind in range(2):
            outs[kind][bottom, columns(index)] += cross_in[index, kind].astype(wide)

    def natural(t, run):
        low, high = due(t)

        def one(index, carry):
            run(index)
            return carry

        lax.fori_loop(low, high, one, 0)

    def step(i, carry):
        @pl.when(i < heads)
        def _():
            compute(i)

        @pl.when(i == min(LAGS[1], DEEP_LAGS[0]))
        def _():
            @pl.when(inner)
            def _():
                pl.semaphore_wait(ready, pairs - 1)
                if direct:
                    greet(at(rim), open_line)

            if direct:
                @pl.when(outer)
                def _():
                    pl.semaphore_wait(open_line, 1)

        def after(lag, run):
            if lag is None:
                return

            @pl.when(jnp.logical_and(i >= lag, i < heads + lag))
            def _():
                run(i - lag)

        after(DEEP_LAGS[0] if deep else None, lambda t: natural(t, deep_merge))
        after(DEEP_LAGS[1] if deep else None, lambda t: natural(t, deep_cross))
        after(LAGS[1], lambda t: natural(t, merge))
        after(LAGS[0], lambda t: relay(head_at(t)))
        after(LAGS[2], lambda t: natural(t, finish))
        after(DEEP_LAGS[2] if deep else None, lambda t: natural(t, deep_finish))
        return carry

    last = heads + max(LAGS[2], DEEP_LAGS[2] if deep else 0)
    lax.fori_loop(0, last, step, 0)

    drain(latents.at[:, :, pl.ds(0, owned), :], latent_send)
    drain(latents.at[pl.ds(0, heads - relief), :, far_rows, :], latent_send)
    for ref in (pair_out, cross_out) if deep else (pair_out,):
        drain(ref, pair_send)

    plain = pl.ds(0, heads - direct)
    if direct:
        drain(direct_out, line_send)

    @pl.when(outer)
    def _():
        drain(edge_out.at[plain], line_send)
        if deep:
            drain(deep_edge_out, line_send)

    @pl.when(inner)
    def _():
        if relief:
            drain(latents.at[pl.ds(0, 2 * relief), :, far_rows, :], latent_send)
        for ref in (near_out.at[plain], far_out.at[plain]) + ((deep_near_out, deep_far_out) if deep else ()):
            drain(ref, line_send)


def attention(images_n, texts_n, order, gate, seen, query, grad, key, value):
    tokens, width = query.shape
    heads = gate.shape[1]
    head_width = width // heads
    rows = key.shape[0] * images_n
    sides = texts_n // 2
    pairs = sides // 2
    share = rows // texts_n
    relief = heads // RELIEF if pairs % 2 == 0 and images_n > 2 else 0
    deep = DEEP if DEEP <= share // 8 else 0
    vmem = pl.BlockSpec(memory_space=pltpu.VMEM)
    hbm = pl.BlockSpec(memory_space=pl.ANY)
    half = jnp.bfloat16
    dma = pltpu.SemaphoreType.DMA((heads,))
    two = pltpu.SemaphoreType.DMA((2, 2))
    pair = pltpu.SemaphoreType.DMA((2,))
    single = pltpu.SemaphoreType.DMA(())
    block = (share - deep, head_width)
    direct = DIRECT if sides <= 4 else 0
    last = pltpu.SemaphoreType.DMA((max(direct, 1), 2))
    small = (max(deep, 8), head_width)
    units = (heads, 2)
    return pl.pallas_call(
        functools.partial(kernel, images_n, sides, relief, direct),
        in_specs=[hbm] * 7,
        out_specs=[vmem, vmem, vmem],
        out_shape=[pltpu.VMEM((tokens, width), half)] + [pltpu.VMEM((share, width), jnp.float32)] * 2,
        scratch_shapes=[
            pltpu.SMEM(order.shape, order.dtype), pltpu.VMEM(gate.shape, gate.dtype), pltpu.VMEM(seen.shape, seen.dtype),
            pltpu.VMEM((order.shape[1], tokens), jnp.float32),
            pltpu.VMEM((heads, tokens, head_width), half),
            pltpu.VMEM((heads, tokens, head_width), half),
            pltpu.VMEM((heads, 2, rows, head_width), half),
            pltpu.VMEM((*units, texts_n, share, head_width), jnp.float32),
            pltpu.VMEM((*units, sides, *block), half),
            pltpu.VMEM((*units, sides, *block), half),
            pltpu.VMEM((*units, sides - 1, *block), half),
            pltpu.VMEM((*units, sides - 1, *block), half),
            pltpu.VMEM((*units, *block), half),
            pltpu.VMEM((*units, *block), half),
            pltpu.VMEM((heads, pairs - 1, 2, 2, *block), half),
            pltpu.VMEM((heads, pairs - 1, 2, *block), half),
            pltpu.VMEM((heads, sides - 1, 2, 2, *small), half),
            pltpu.VMEM((heads, sides - 1, 2, 2, *small), half),
            pltpu.VMEM((heads, 2, 2, *small), half),
            pltpu.VMEM((heads, 2, 2, *small), half),
            pltpu.VMEM((heads, pairs - 1, 2, 2, 2, *small), half),
            pltpu.VMEM((heads, pairs - 1, 2, 2, *small), half),
            pltpu.VMEM((*units, *small), half),
            pltpu.VMEM((*units, *small), half),
            pltpu.VMEM((max(direct, 1), 2, sides - 1, *block), half),
            pltpu.VMEM((max(direct, 1), 2, sides - 1, *block), half),
            pltpu.VMEM((images_n - 2, 2, rows // images_n, head_width), half),
            two, pair, dma, single, single, dma, single, dma, last, dma,
            dma, dma, dma, last, pltpu.SemaphoreType.DMA((4,)),
            pltpu.SemaphoreType.REGULAR, pltpu.SemaphoreType.REGULAR,
        ],
        compiler_params=pltpu.CompilerParams(
            vmem_limit_bytes=56 * 1024 * 1024, collective_id=0, has_side_effects=True
        ),
    )(order, gate, seen, query, grad, key, value)


def publish(*arrays):
    def body(*refs):
        count = len(arrays)
        sems = refs[-1]
        copies = [pltpu.make_async_copy(refs[n], refs[count + n], sems.at[n]) for n in range(count)]
        for copy in copies:
            copy.start()
        for copy in copies:
            copy.wait()

    return pl.pallas_call(
        body,
        in_specs=[pl.BlockSpec(memory_space=pltpu.VMEM)] * len(arrays),
        out_specs=[pl.BlockSpec(memory_space=pl.ANY)] * len(arrays),
        out_shape=[jax.ShapeDtypeStruct(array.shape, array.dtype) for array in arrays],
        scratch_shapes=[pltpu.SemaphoreType.DMA((len(arrays),))],
        compiler_params=pltpu.CompilerParams(vmem_limit_bytes=1024 * 1024),
    )(*[pltpu.with_memory_space_constraint(array, pltpu.VMEM) for array in arrays])


def shards(images_n, texts_n, queries, visual_keys, visual_values, out_grad, gate_value, image_order, image_seen):
    query_grad, key_share, value_share = publish(*attention(
        images_n, texts_n, image_order, gate_value, image_seen,
        queries[0], out_grad[0], visual_keys[0], visual_values[0]
    ))
    return (query_grad[None], key_share[None], value_share[None])


def solution(mesh):
    placed = (
        P(None, "txt", "img"),
        P(None, "img", None),
        P(None, "img", None),
        P(None, "txt", "img"),
        P(None, "img"),
        P(),
        P("txt"),
    )
    return jax.shard_map(
        functools.partial(shards, mesh.shape["img"], mesh.shape["txt"]),
        mesh=mesh,
        in_specs=placed,
        out_specs=(P(None, "txt", "img"), P(None, "txt", "img"), P(None, "txt", "img")),
        check_vma=False,
    )
```

```python
import functools
import math

import jax
import jax.numpy as jnp
from jax import lax
from jax.experimental import pallas as pl
from jax.experimental.pallas import tpu as pltpu
from jax.sharding import PartitionSpec as P

NT = (((1,), (1,)), ((), ()))
TN = (((0,), (0,)), ((), ()))
NN = (((1,), (0,)), ((), ()))
MESH = pl.DeviceIdType.MESH
LAGS = (2, 4, 6)
DEEP_LAGS = (2, 4, 7)
RELIEF = 5
DEEP = 8
DIRECT = 1


def matmul(left, right, dims):
    return lax.dot_general(left, right, dims, preferred_element_type=jnp.float32)


def head_grads(query, gated, key, value, bias):
    rows, tokens = key.shape[0], query.shape[0]
    images = bias.shape[0]
    scale = 1.0 / math.sqrt(query.shape[1])
    scores = matmul(key, query, NT) * (scale * math.log2(math.e))
    masked = (scores.reshape(images, rows // images, tokens) + bias[:, None, :]).reshape(rows, tokens)
    exponent = jnp.exp2(masked - jnp.max(masked, axis=0, keepdims=True))
    weights = exponent * (1.0 / jnp.sum(exponent, axis=0, keepdims=True))
    weight_half = weights.astype(jnp.bfloat16)
    weight_grad = matmul(value, gated, NT)
    delta = jnp.sum(weight_half.astype(jnp.float32) * weight_grad, axis=0, keepdims=True)
    score_half = (weights * (weight_grad - delta)).astype(jnp.bfloat16)
    query_grad = (matmul(key, score_half, TN) * scale).T
    key_grad = matmul(score_half, query, NN) * scale
    value_grad = matmul(weight_half, gated, NN)
    return query_grad, key_grad, value_grad


def kernel(images_n, sides, relief, direct, order_hbm, gate_hbm, seen_hbm, query_ref, grad_ref, key_ref, value_ref,
           out_ref, key_out, value_out,
           order_ref, gate_ref, seen_ref, bias, queries, grads, latents, full, pair_out, pair_in, edge_out, edge_in, near_out, near_in,
           far_out, far_in, deep_edge_out, deep_edge_in, deep_near_out, deep_near_in, deep_far_out, deep_far_in,
           cross_out, cross_in, direct_out, direct_in, first,
           load_sem, near_sem, far_sem, latent_send, pair_send, pair_recv, line_send, line_recv, last_recv,
           far_recv, deep_line, deep_far, deep_cross_recv, direct_recv, own_sem, ready, open_line):
    heads = gate_ref.shape[1]
    width = queries.shape[2]
    owned = key_ref.shape[0]
    half = jnp.bfloat16
    wide = jnp.float32
    pairs = sides // 2
    chips = images_n // 2
    me = lax.axis_index("img")
    place = lax.axis_index("txt")
    mine = place // 2
    side = place % 2
    other = 1 - side
    group = mine // 2
    parity = group % 2

    def hub_of(g):
        return g * 2 + (jnp.where(g < pairs // 2, 1, 0) if pairs > 1 else 1)

    hub = hub_of(group)
    rim = group * 4 + 1 - hub
    inner = mine == hub
    outer = mine == rim
    chip = me // 2
    sibling = chip * 2 + 1 - me % 2
    across = {"txt": mine * 2 + other}

    def at(z):
        return {"txt": z * 2 + side}

    def columns(index):
        return pl.ds(pl.multiple_of(index * width, width), width)

    def remote(src, dst, send, recv, device):
        return pltpu.make_async_remote_copy(src_ref=src, dst_ref=dst, send_sem=send, recv_sem=recv,
                                            device_id=device, device_id_type=MESH)

    def drain(ref, sem):
        pltpu.make_async_copy(ref, ref, sem).wait()

    def rows_of(owner, count):
        return pl.ds(pl.multiple_of(owner * owned, owned), count * owned)

    takes = jnp.where(inner, parity, 1 - parity)

    def relieved(index):
        return jnp.logical_and(index >= 1, index <= 2 * relief)

    def fetched(index):
        return jnp.logical_or(jnp.logical_not(relieved(index)), (index + 1) % 2 == takes)

    def forwarder(index):
        return jnp.logical_and(inner, jnp.logical_and(relieved(index), fetched(index)))

    def head_at(i):
        k = i // 2
        taken = jnp.where(i == 1, 1 + takes, 2 * k + 1 + takes)
        handed = 2 * k - takes
        late = jnp.logical_or(jnp.logical_and(i % 2 == 1, i > 1), i == 2 * relief)
        return jnp.where(relieved(i), jnp.where(late, handed, taken), i)

    def due(t):
        k = t // 2
        late = jnp.logical_or(jnp.logical_and(t % 2 == 1, t > 1), t == 2 * relief)
        low = jnp.where(relieved(t), 2 * k - 1, t)
        high = jnp.where(relieved(t), jnp.where(late, low + 2, low), t + 1)
        return low, high

    share = full.shape[3]
    deep = cross_out.shape[2] if DEEP <= share // 8 else 0
    top = pl.ds(0, share - deep)
    bottom = pl.ds(share - deep, deep)

    def forward_copies(index):
        copies = []
        for device in (at(hub_of(group ^ 1)), at(rim)):
            for off in range(1, chips):
                view = latents.at[index, :, rows_of(((chip + off) % chips) * 2, 2), :]
                copies.append(remote(view, view, latent_send, far_sem.at[index], device))
        return copies

    def pair_copy(index):
        return remote(pair_out.at[index], pair_in.at[index], pair_send, pair_recv.at[index], across)

    def last_copy(index, kind):
        return remote(pair_out.at[index, kind], pair_in.at[index, kind],
                      pair_send, last_recv.at[index - (heads - direct), kind], across)

    def cross_copy(index):
        return remote(cross_out.at[index], cross_in.at[index], pair_send, deep_cross_recv.at[index], across)

    def edge_copy(index):
        return remote(edge_out.at[index], edge_in.at[index], line_send, line_recv.at[index], at(hub))

    def near_copy(index):
        return remote(near_out.at[index], near_in.at[index], line_send, line_recv.at[index], at(rim))

    def far_copy(index, off, member):
        return remote(far_out.at[index, off - 1, member], far_in.at[index, off - 1],
                      line_send, far_recv.at[index], at(((group + off) % pairs) * 2 + member))

    def deep_edge_copy(index):
        return remote(deep_edge_out.at[index], deep_edge_in.at[index], line_send, deep_line.at[index], at(hub))

    def deep_near_copy(index):
        return remote(deep_near_out.at[index], deep_near_in.at[index], line_send, deep_line.at[index], at(rim))

    def deep_far_copy(index, off, member):
        return remote(deep_far_out.at[index, off - 1, member], deep_far_in.at[index, off - 1],
                      line_send, deep_far.at[index], at(((group + off) % pairs) * 2 + member))

    barrier = pltpu.get_barrier_semaphore()

    def greet(device, semaphore=barrier):
        pl.semaphore_signal(semaphore, inc=1, device_id=device, device_id_type=MESH)

    for off in range(1, images_n):
        greet({"img": (me + off) % images_n})
    greet(across)
    greet(at(mine ^ 1))

    @pl.when(inner)
    def _():
        for off in range(1, pairs):
            greet(at(hub_of((group + off) % pairs)))

    small = [pltpu.make_async_copy(ref, buf, own_sem.at[n]) for n, (ref, buf) in enumerate(
        ((order_hbm, order_ref), (gate_hbm, gate_ref), (seen_hbm, seen_ref)))]

    def rest(index):
        return jnp.minimum(index, 1)

    def load(index):
        return [pltpu.make_async_copy(ref.at[:, columns(index)], buf.at[index], load_sem.at[n, rest(index)])
                for n, (ref, buf) in enumerate(((query_ref, queries), (grad_ref, grads)))]

    sources = (key_ref, value_ref)
    strangers = [((chip + off) % chips) * 2 + core for off in range(1, chips) for core in range(2)]
    staged = [pltpu.make_async_copy(ref.at[:, columns(owner * heads)], first.at[n, kind], own_sem.at[3])
              for n, owner in enumerate(strangers) for kind, ref in enumerate(sources)]
    for copy in staged + small + load(0):
        copy.start()
    drain(first, own_sem.at[3])
    pl.semaphore_wait(barrier, images_n + 1 + (pairs - 1) * jnp.where(inner, 1, 0))

    @pl.when(inner)
    def _():
        for off in range(1, pairs):
            greet(at(hub_of((group + off) % pairs)), ready)

    def latent_copy(index, owner, kind, sem, source=None):
        source = sources[kind].at[:, columns(owner * heads + index)] if source is None else source
        return remote(source,
                      latents.at[index, kind, rows_of(me, 1), :],
                      latent_send, sem, {"img": owner})

    def send(index, carry):
        @pl.when(jnp.logical_and(index > 0, fetched(index)))
        def _():
            for owner in strangers:
                for kind in range(2):
                    latent_copy(index, owner, kind, far_sem.at[index]).start()

        for kind, ref in enumerate(sources):
            latent_copy(index, sibling, kind, near_sem.at[rest(index)]).start()
            pltpu.make_async_copy(ref.at[:, columns(me * heads + index)],
                                  latents.at[index, kind, rows_of(me, 1), :], near_sem.at[rest(index)]).start()

        @pl.when(index > 0)
        def _():
            for copy in load(index):
                copy.start()

        return carry

    for n, owner in enumerate(strangers):
        for kind in range(2):
            latent_copy(0, owner, kind, far_sem.at[0], first.at[n, kind]).start()
    lax.fori_loop(0, heads, send, 0)
    for copy in small:
        copy.wait()
    seen = seen_ref[...].reshape(1, bias.shape[1])
    for i in range(order_ref.shape[1]):
        bias[pl.ds(i, 1), :] = jnp.where(seen > order_ref[0, i], 0.0, -1e30)

    outs = (key_out, value_out)
    far_rows = pl.ds(0, (images_n - 2) * owned)

    def arrive(part, count):
        drain(latents.at[pl.ds(0, count), :, pl.ds(0, 2 * owned), :], near_sem.at[part])
        for n, buf in enumerate((queries, grads)):
            drain(buf.at[pl.ds(0, count)], load_sem.at[n, part])

    def compute(i):
        index = head_at(i)

        @pl.when(i == 0)
        def _():
            arrive(0, 1)

        @pl.when(i == 1)
        def _():
            arrive(1, heads - 1)

        drain(latents.at[index, :, far_rows, :], far_sem.at[index])

        @pl.when(forwarder(index))
        def _():
            for copy in forward_copies(index):
                copy.start()

        lane = lax.broadcasted_iota(jnp.int32, gate_ref.shape, 1)
        gate = jnp.sum(jnp.where(lane == index, gate_ref[...], 0.0), axis=1, keepdims=True)
        gated = (grads[index].astype(wide) * jnp.tanh(gate)).astype(half)
        query_grad, key_grad, value_grad = head_grads(
            queries[index], gated, latents[index, 0], latents[index, 1], bias[...]
        )
        out_ref[:, columns(index)] = query_grad.astype(out_ref.dtype)
        shape = full.shape[2:]
        full[index, 0] = key_grad.reshape(shape)
        full[index, 1] = value_grad.reshape(shape)

        for kind in (1, 0):
            for z in range(sides):
                pair_out[index, kind, z] = full[index, kind, z * 2 + other, top].astype(half)
            if direct:
                @pl.when(straight(index))
                def _():
                    last_copy(index, kind).start()

        @pl.when(jnp.logical_not(straight(index)))
        def _():
            pair_copy(index).start()

        if deep:
            @pl.when(outer)
            def _():
                for kind in range(2):
                    for j in range(sides - 1):
                        for x in range(2):
                            deep_edge_out[index, j, x, kind] = (
                                full[index, kind, ((rim + 1 + j) % sides) * 2 + x, bottom].astype(half)
                            )
                deep_edge_copy(index).start()

            @pl.when(inner)
            def _():
                for kind in range(2):
                    for x in range(2):
                        deep_near_out[index, x, kind] = full[index, kind, rim * 2 + x, bottom].astype(half)
                deep_near_copy(index).start()

    def line(index, kind, z):
        return full[index, kind, z * 2 + side, top] + pair_in[index, kind, z].astype(wide)

    def straight(index):
        return index >= heads - direct

    def direct_copy(index, kind, off):
        n = index - (heads - direct)
        return remote(direct_out.at[n, kind, off - 1], direct_in.at[n, kind, off - 1],
                      line_send, direct_recv.at[n, kind], at((mine + off) % sides))

    def relay(index):
        @pl.when(jnp.logical_not(straight(index)))
        def _():
            pair_copy(index).wait_recv()

            @pl.when(outer)
            def _():
                for kind in range(2):
                    for j in range(sides - 1):
                        edge_out[index, kind, j] = line(index, kind, (rim + 1 + j) % sides).astype(half)
                edge_copy(index).start()

            @pl.when(inner)
            def _():
                for kind in range(2):
                    near_out[index, kind] = line(index, kind, rim).astype(half)
                near_copy(index).start()

            for kind in range(2):
                outs[kind][top, columns(index)] = line(index, kind, mine)

        if direct:
            @pl.when(straight(index))
            def _():
                for kind in (1, 0):
                    last_copy(index, kind).wait_recv()
                    for off in range(1, sides):
                        direct_out[index - (heads - direct), kind, off - 1] = (
                            line(index, kind, (mine + off) % sides).astype(half)
                        )
                        direct_copy(index, kind, off).start()
                    outs[kind][top, columns(index)] = line(index, kind, mine)

    mid = (hub - rim - 1 + sides) % sides

    def merge(index):
        @pl.when(jnp.logical_and(inner, jnp.logical_not(straight(index))))
        def _():
            edge_copy(index).wait_recv()
            for off in range(1, pairs):
                for member in range(2):
                    z = ((group + off) % pairs) * 2 + member
                    for kind in range(2):
                        far_out[index, off - 1, member, kind] = (
                            line(index, kind, z) + edge_in[index, kind, (z - rim - 1 + sides) % sides].astype(wide)
                        ).astype(half)
                    far_copy(index, off, member).start()
            for kind in range(2):
                outs[kind][top, columns(index)] += edge_in[index, kind, mid].astype(wide)

        @pl.when(jnp.logical_and(outer, jnp.logical_not(straight(index))))
        def _():
            near_copy(index).wait_recv()
            for kind in range(2):
                outs[kind][top, columns(index)] += near_in[index, kind].astype(wide)

    def gather(index, kind, terms):
        total = outs[kind][top, columns(index)]
        for term in terms:
            total = total + term.astype(wide)
        outs[kind][top, columns(index)] = total

    def finish(index):
        @pl.when(jnp.logical_not(straight(index)))
        def _():
            drain(far_in.at[index], far_recv.at[index])
            for kind in range(2):
                gather(index, kind, [far_in[index, n, kind] for n in range(pairs - 1)])

        if direct:
            @pl.when(straight(index))
            def _():
                n = index - (heads - direct)
                for kind in (1, 0):
                    drain(direct_in.at[n, kind], direct_recv.at[n, kind])
                    gather(index, kind, [direct_in[n, kind, off] for off in range(sides - 1)])

    def deep_merge(index):
        @pl.when(inner)
        def _():
            deep_edge_copy(index).wait_recv()
            for off in range(1, pairs):
                for member in range(2):
                    z = ((group + off) % pairs) * 2 + member
                    for kind in range(2):
                        for x in range(2):
                            deep_far_out[index, off - 1, member, x, kind] = (
                                full[index, kind, z * 2 + x, bottom]
                                + deep_edge_in[index, (z - rim - 1 + sides) % sides, x, kind].astype(wide)
                            ).astype(half)
                    deep_far_copy(index, off, member).start()
            for kind in range(2):
                for x in range(2):
                    full[index, kind, mine * 2 + x, bottom] += deep_edge_in[index, mid, x, kind].astype(wide)

        @pl.when(outer)
        def _():
            deep_near_copy(index).wait_recv()
            for kind in range(2):
                for x in range(2):
                    full[index, kind, mine * 2 + x, bottom] += deep_near_in[index, x, kind].astype(wide)

    def deep_cross(index):
        drain(deep_far_in.at[index], deep_far.at[index])

        def total(kind, x):
            value = full[index, kind, mine * 2 + x, bottom]
            for off in range(1, pairs):
                value = value + deep_far_in[index, off - 1, x, kind].astype(wide)
            return value

        for kind in range(2):
            cross_out[index, kind] = total(kind, other).astype(half)
        cross_copy(index).start()
        for kind in range(2):
            outs[kind][bottom, columns(index)] = total(kind, side)

    def deep_finish(index):
        cross_copy(index).wait_recv()
        for kind in range(2):
            outs[kind][bottom, columns(index)] += cross_in[index, kind].astype(wide)

    def natural(t, run):
        low, high = due(t)

        def one(index, carry):
            run(index)
            return carry

        lax.fori_loop(low, high, one, 0)

    def step(i, carry):
        @pl.when(i < heads)
        def _():
            compute(i)

        @pl.when(i == min(LAGS[1], DEEP_LAGS[0]))
        def _():
            @pl.when(inner)
            def _():
                pl.semaphore_wait(ready, pairs - 1)
                if direct:
                    greet(at(rim), open_line)

            if direct:
                @pl.when(outer)
                def _():
                    pl.semaphore_wait(open_line, 1)

        def after(lag, run):
            if lag is None:
                return

            @pl.when(jnp.logical_and(i >= lag, i < heads + lag))
            def _():
                run(i - lag)

        after(DEEP_LAGS[0] if deep else None, lambda t: natural(t, deep_merge))
        after(DEEP_LAGS[1] if deep else None, lambda t: natural(t, deep_cross))
        after(LAGS[1], lambda t: natural(t, merge))
        after(LAGS[0], lambda t: relay(head_at(t)))
        after(LAGS[2], lambda t: natural(t, finish))
        after(DEEP_LAGS[2] if deep else None, lambda t: natural(t, deep_finish))
        return carry

    last = heads + max(LAGS[2], DEEP_LAGS[2] if deep else 0)
    lax.fori_loop(0, last, step, 0)

    drain(latents.at[:, :, pl.ds(0, owned), :], latent_send)
    drain(latents.at[pl.ds(0, heads - relief), :, far_rows, :], latent_send)
    for ref in (pair_out, cross_out) if deep else (pair_out,):
        drain(ref, pair_send)

    plain = pl.ds(0, heads - direct)
    if direct:
        drain(direct_out, line_send)

    @pl.when(outer)
    def _():
        drain(edge_out.at[plain], line_send)
        if deep:
            drain(deep_edge_out, line_send)

    @pl.when(inner)
    def _():
        if relief:
            drain(latents.at[pl.ds(0, 2 * relief), :, far_rows, :], latent_send)
        for ref in (near_out.at[plain], far_out.at[plain]) + ((deep_near_out, deep_far_out) if deep else ()):
            drain(ref, line_send)


def attention(images_n, texts_n, order, gate, seen, query, grad, key, value):
    tokens, width = query.shape
    heads = gate.shape[1]
    head_width = width // heads
    rows = key.shape[0] * images_n
    sides = texts_n // 2
    pairs = sides // 2
    share = rows // texts_n
    relief = heads // RELIEF if pairs % 2 == 0 and images_n > 2 else 0
    deep = DEEP if DEEP <= share // 8 else 0
    vmem = pl.BlockSpec(memory_space=pltpu.VMEM)
    hbm = pl.BlockSpec(memory_space=pl.ANY)
    half = jnp.bfloat16
    dma = pltpu.SemaphoreType.DMA((heads,))
    two = pltpu.SemaphoreType.DMA((2, 2))
    pair = pltpu.SemaphoreType.DMA((2,))
    single = pltpu.SemaphoreType.DMA(())
    block = (share - deep, head_width)
    direct = DIRECT if sides <= 4 else 0
    last = pltpu.SemaphoreType.DMA((max(direct, 1), 2))
    small = (max(deep, 8), head_width)
    units = (heads, 2)
    return pl.pallas_call(
        functools.partial(kernel, images_n, sides, relief, direct),
        in_specs=[hbm] * 7,
        out_specs=[vmem, vmem, vmem],
        out_shape=[pltpu.VMEM((tokens, width), half)] + [pltpu.VMEM((share, width), jnp.float32)] * 2,
        scratch_shapes=[
            pltpu.SMEM(order.shape, order.dtype), pltpu.VMEM(gate.shape, gate.dtype), pltpu.VMEM(seen.shape, seen.dtype),
            pltpu.VMEM((order.shape[1], tokens), jnp.float32),
            pltpu.VMEM((heads, tokens, head_width), half),
            pltpu.VMEM((heads, tokens, head_width), half),
            pltpu.VMEM((heads, 2, rows, head_width), half),
            pltpu.VMEM((*units, texts_n, share, head_width), jnp.float32),
            pltpu.VMEM((*units, sides, *block), half),
            pltpu.VMEM((*units, sides, *block), half),
            pltpu.VMEM((*units, sides - 1, *block), half),
            pltpu.VMEM((*units, sides - 1, *block), half),
            pltpu.VMEM((*units, *block), half),
            pltpu.VMEM((*units, *block), half),
            pltpu.VMEM((heads, pairs - 1, 2, 2, *block), half),
            pltpu.VMEM((heads, pairs - 1, 2, *block), half),
            pltpu.VMEM((heads, sides - 1, 2, 2, *small), half),
            pltpu.VMEM((heads, sides - 1, 2, 2, *small), half),
            pltpu.VMEM((heads, 2, 2, *small), half),
            pltpu.VMEM((heads, 2, 2, *small), half),
            pltpu.VMEM((heads, pairs - 1, 2, 2, 2, *small), half),
            pltpu.VMEM((heads, pairs - 1, 2, 2, *small), half),
            pltpu.VMEM((*units, *small), half),
            pltpu.VMEM((*units, *small), half),
            pltpu.VMEM((max(direct, 1), 2, sides - 1, *block), half),
            pltpu.VMEM((max(direct, 1), 2, sides - 1, *block), half),
            pltpu.VMEM((images_n - 2, 2, rows // images_n, head_width), half),
            two, pair, dma, single, single, dma, single, dma, last, dma,
            dma, dma, dma, last, pltpu.SemaphoreType.DMA((4,)),
            pltpu.SemaphoreType.REGULAR, pltpu.SemaphoreType.REGULAR,
        ],
        compiler_params=pltpu.CompilerParams(
            vmem_limit_bytes=56 * 1024 * 1024, collective_id=0, has_side_effects=True
        ),
    )(order, gate, seen, query, grad, key, value)


def publish(*arrays):
    def body(*refs):
        count = len(arrays)
        sems = refs[-1]
        copies = [pltpu.make_async_copy(refs[n], refs[count + n], sems.at[n]) for n in range(count)]
        for copy in copies:
            copy.start()
        for copy in copies:
            copy.wait()

    return pl.pallas_call(
        body,
        in_specs=[pl.BlockSpec(memory_space=pltpu.VMEM)] * len(arrays),
        out_specs=[pl.BlockSpec(memory_space=pl.ANY)] * len(arrays),
        out_shape=[jax.ShapeDtypeStruct(array.shape, array.dtype) for array in arrays],
        scratch_shapes=[pltpu.SemaphoreType.DMA((len(arrays),))],
        compiler_params=pltpu.CompilerParams(vmem_limit_bytes=1024 * 1024),
    )(*[pltpu.with_memory_space_constraint(array, pltpu.VMEM) for array in arrays])


def shards(images_n, texts_n, queries, visual_keys, visual_values, out_grad, gate_value, image_order, image_seen):
    query_grad, key_share, value_share = publish(*attention(
        images_n, texts_n, image_order, gate_value, image_seen,
        queries[0], out_grad[0], visual_keys[0], visual_values[0]
    ))
    return (query_grad[None], key_share[None], value_share[None])


def solution(mesh):
    placed = (
        P(None, "txt", "img"),
        P(None, "img", None),
        P(None, "img", None),
        P(None, "txt", "img"),
        P(None, "img"),
        P(),
        P("txt"),
    )
    return jax.shard_map(
        functools.partial(shards, mesh.shape["img"], mesh.shape["txt"]),
        mesh=mesh,
        in_specs=placed,
        out_specs=(P(None, "txt", "img"), P(None, "txt", "img"), P(None, "txt", "img")),
        check_vma=False,
    )
```

```python
import functools
import math

import jax
import jax.numpy as jnp
from jax import lax
from jax.experimental import pallas as pl
from jax.experimental.pallas import tpu as pltpu
from jax.sharding import PartitionSpec as P

NT = (((1,), (1,)), ((), ()))
TN = (((0,), (0,)), ((), ()))
NN = (((1,), (0,)), ((), ()))
MESH = pl.DeviceIdType.MESH
LAGS = (2, 4, 6)
DEEP_LAGS = (2, 4, 7)
RELIEF = 5
DEEP = 8
DIRECT = 1


def matmul(left, right, dims):
    return lax.dot_general(left, right, dims, preferred_element_type=jnp.float32)


def head_grads(query, gated, key, value, bias):
    rows, tokens = key.shape[0], query.shape[0]
    images = bias.shape[0]
    scale = 1.0 / math.sqrt(query.shape[1])
    scores = matmul(key, query, NT) * (scale * math.log2(math.e))
    masked = (scores.reshape(images, rows // images, tokens) + bias[:, None, :]).reshape(rows, tokens)
    exponent = jnp.exp2(masked - jnp.max(masked, axis=0, keepdims=True))
    weights = exponent * (1.0 / jnp.sum(exponent, axis=0, keepdims=True))
    weight_half = weights.astype(jnp.bfloat16)
    weight_grad = matmul(value, gated, NT)
    delta = jnp.sum(weight_half.astype(jnp.float32) * weight_grad, axis=0, keepdims=True)
    score_half = (weights * (weight_grad - delta)).astype(jnp.bfloat16)
    query_grad = (matmul(key, score_half, TN) * scale).T
    key_grad = matmul(score_half, query, NN) * scale
    value_grad = matmul(weight_half, gated, NN)
    return query_grad, key_grad, value_grad


def kernel(images_n, sides, relief, direct, order_hbm, gate_hbm, seen_hbm, query_ref, grad_ref, key_ref, value_ref,
           out_ref, key_out, value_out,
           order_ref, gate_ref, seen_ref, bias, queries, grads, latents, full, pair_out, pair_in, edge_out, edge_in, near_out, near_in,
           far_out, far_in, deep_edge_out, deep_edge_in, deep_near_out, deep_near_in, deep_far_out, deep_far_in,
           cross_out, cross_in, direct_out, direct_in, first,
           load_sem, near_sem, far_sem, latent_send, pair_send, pair_recv, line_send, line_recv, last_recv,
           far_recv, deep_line, deep_far, deep_cross_recv, direct_recv, own_sem, ready, open_line):
    heads = gate_ref.shape[1]
    width = queries.shape[2]
    owned = key_ref.shape[0]
    half = jnp.bfloat16
    wide = jnp.float32
    pairs = sides // 2
    chips = images_n // 2
    me = lax.axis_index("img")
    place = lax.axis_index("txt")
    mine = place // 2
    side = place % 2
    other = 1 - side
    group = mine // 2
    parity = group % 2

    def hub_of(g):
        return g * 2 + (jnp.where(g < pairs // 2, 1, 0) if pairs > 1 else 1)

    hub = hub_of(group)
    rim = group * 4 + 1 - hub
    inner = mine == hub
    outer = mine == rim
    chip = me // 2
    sibling = chip * 2 + 1 - me % 2
    across = {"txt": mine * 2 + other}

    def at(z):
        return {"txt": z * 2 + side}

    def columns(index):
        return pl.ds(pl.multiple_of(index * width, width), width)

    def remote(src, dst, send, recv, device):
        return pltpu.make_async_remote_copy(src_ref=src, dst_ref=dst, send_sem=send, recv_sem=recv,
                                            device_id=device, device_id_type=MESH)

    def drain(ref, sem):
        pltpu.make_async_copy(ref, ref, sem).wait()

    def rows_of(owner, count):
        return pl.ds(pl.multiple_of(owner * owned, owned), count * owned)

    takes = jnp.where(inner, parity, 1 - parity)

    def relieved(index):
        return jnp.logical_and(index >= 1, index <= 2 * relief)

    def fetched(index):
        return jnp.logical_or(jnp.logical_not(relieved(index)), (index + 1) % 2 == takes)

    def forwarder(index):
        return jnp.logical_and(inner, jnp.logical_and(relieved(index), fetched(index)))

    def head_at(i):
        k = i // 2
        taken = jnp.where(i == 1, 1 + takes, 2 * k + 1 + takes)
        handed = 2 * k - takes
        late = jnp.logical_or(jnp.logical_and(i % 2 == 1, i > 1), i == 2 * relief)
        return jnp.where(relieved(i), jnp.where(late, handed, taken), i)

    def due(t):
        k = t // 2
        late = jnp.logical_or(jnp.logical_and(t % 2 == 1, t > 1), t == 2 * relief)
        low = jnp.where(relieved(t), 2 * k - 1, t)
        high = jnp.where(relieved(t), jnp.where(late, low + 2, low), t + 1)
        return low, high

    share = full.shape[3]
    deep = cross_out.shape[2] if DEEP <= share // 8 else 0
    top = pl.ds(0, share - deep)
    bottom = pl.ds(share - deep, deep)

    def forward_copies(index):
        copies = []
        for device in (at(hub_of(group ^ 1)), at(rim)):
            for off in range(1, chips):
                view = latents.at[index, :, rows_of(((chip + off) % chips) * 2, 2), :]
                copies.append(remote(view, view, latent_send, far_sem.at[index], device))
        return copies

    def pair_copy(index):
        return remote(pair_out.at[index], pair_in.at[index], pair_send, pair_recv.at[index], across)

    def last_copy(index, kind):
        return remote(pair_out.at[index, kind], pair_in.at[index, kind],
                      pair_send, last_recv.at[index - (heads - direct), kind], across)

    def cross_copy(index):
        return remote(cross_out.at[index], cross_in.at[index], pair_send, deep_cross_recv.at[index], across)

    def edge_copy(index):
        return remote(edge_out.at[index], edge_in.at[index], line_send, line_recv.at[index], at(hub))

    def near_copy(index):
        return remote(near_out.at[index], near_in.at[index], line_send, line_recv.at[index], at(rim))

    def far_copy(index, off, member):
        return remote(far_out.at[index, off - 1, member], far_in.at[index, off - 1],
                      line_send, far_recv.at[index], at(((group + off) % pairs) * 2 + member))

    def deep_edge_copy(index):
        return remote(deep_edge_out.at[index], deep_edge_in.at[index], line_send, deep_line.at[index], at(hub))

    def deep_near_copy(index):
        return remote(deep_near_out.at[index], deep_near_in.at[index], line_send, deep_line.at[index], at(rim))

    def deep_far_copy(index, off, member):
        return remote(deep_far_out.at[index, off - 1, member], deep_far_in.at[index, off - 1],
                      line_send, deep_far.at[index], at(((group + off) % pairs) * 2 + member))

    barrier = pltpu.get_barrier_semaphore()

    def greet(device, semaphore=barrier):
        pl.semaphore_signal(semaphore, inc=1, device_id=device, device_id_type=MESH)

    for off in range(1, images_n):
        greet({"img": (me + off) % images_n})
    greet(across)
    greet(at(mine ^ 1))

    @pl.when(inner)
    def _():
        for off in range(1, pairs):
            greet(at(hub_of((group + off) % pairs)))

    small = [pltpu.make_async_copy(ref, buf, own_sem.at[n]) for n, (ref, buf) in enumerate(
        ((order_hbm, order_ref), (gate_hbm, gate_ref), (seen_hbm, seen_ref)))]

    def rest(index):
        return jnp.minimum(index, 1)

    def load(index):
        return [pltpu.make_async_copy(ref.at[:, columns(index)], buf.at[index], load_sem.at[n, rest(index)])
                for n, (ref, buf) in enumerate(((query_ref, queries), (grad_ref, grads)))]

    sources = (key_ref, value_ref)
    strangers = [((chip + off) % chips) * 2 + core for off in range(1, chips) for core in range(2)]
    staged = [pltpu.make_async_copy(ref.at[:, columns(owner * heads)], first.at[n, kind], own_sem.at[3])
              for n, owner in enumerate(strangers) for kind, ref in enumerate(sources)]
    for copy in staged + small + load(0):
        copy.start()
    drain(first, own_sem.at[3])
    pl.semaphore_wait(barrier, images_n + 1 + (pairs - 1) * jnp.where(inner, 1, 0))

    @pl.when(inner)
    def _():
        for off in range(1, pairs):
            greet(at(hub_of((group + off) % pairs)), ready)

    def latent_copy(index, owner, kind, sem, source=None):
        source = sources[kind].at[:, columns(owner * heads + index)] if source is None else source
        return remote(source,
                      latents.at[index, kind, rows_of(me, 1), :],
                      latent_send, sem, {"img": owner})

    def send(index, carry):
        @pl.when(jnp.logical_and(index > 0, fetched(index)))
        def _():
            for owner in strangers:
                for kind in range(2):
                    latent_copy(index, owner, kind, far_sem.at[index]).start()

        for kind, ref in enumerate(sources):
            latent_copy(index, sibling, kind, near_sem.at[rest(index)]).start()
            pltpu.make_async_copy(ref.at[:, columns(me * heads + index)],
                                  latents.at[index, kind, rows_of(me, 1), :], near_sem.at[rest(index)]).start()

        @pl.when(index > 0)
        def _():
            for copy in load(index):
                copy.start()

        return carry

    for n, owner in enumerate(strangers):
        for kind in range(2):
            latent_copy(0, owner, kind, far_sem.at[0], first.at[n, kind]).start()
    lax.fori_loop(0, heads, send, 0)
    for copy in small:
        copy.wait()
    seen = seen_ref[...].reshape(1, bias.shape[1])
    for i in range(order_ref.shape[1]):
        bias[pl.ds(i, 1), :] = jnp.where(seen > order_ref[0, i], 0.0, -1e30)

    outs = (key_out, value_out)
    far_rows = pl.ds(0, (images_n - 2) * owned)

    def arrive(part, count):
        drain(latents.at[pl.ds(0, count), :, pl.ds(0, 2 * owned), :], near_sem.at[part])
        for n, buf in enumerate((queries, grads)):
            drain(buf.at[pl.ds(0, count)], load_sem.at[n, part])

    def compute(i):
        index = head_at(i)

        @pl.when(i == 0)
        def _():
            arrive(0, 1)

        @pl.when(i == 1)
        def _():
            arrive(1, heads - 1)

        drain(latents.at[index, :, far_rows, :], far_sem.at[index])

        @pl.when(forwarder(index))
        def _():
            for copy in forward_copies(index):
                copy.start()

        lane = lax.broadcasted_iota(jnp.int32, gate_ref.shape, 1)
        gate = jnp.sum(jnp.where(lane == index, gate_ref[...], 0.0), axis=1, keepdims=True)
        gated = (grads[index].astype(wide) * jnp.tanh(gate)).astype(half)
        query_grad, key_grad, value_grad = head_grads(
            queries[index], gated, latents[index, 0], latents[index, 1], bias[...]
        )
        out_ref[:, columns(index)] = query_grad.astype(out_ref.dtype)
        shape = full.shape[2:]
        full[index, 0] = key_grad.reshape(shape)
        full[index, 1] = value_grad.reshape(shape)

        for kind in (1, 0):
            for z in range(sides):
                pair_out[index, kind, z] = full[index, kind, z * 2 + other, top].astype(half)
            if direct:
                @pl.when(straight(index))
                def _():
                    last_copy(index, kind).start()

        @pl.when(jnp.logical_not(straight(index)))
        def _():
            pair_copy(index).start()

        if deep:
            @pl.when(outer)
            def _():
                for kind in range(2):
                    for j in range(sides - 1):
                        for x in range(2):
                            deep_edge_out[index, j, x, kind] = (
                                full[index, kind, ((rim + 1 + j) % sides) * 2 + x, bottom].astype(half)
                            )
                deep_edge_copy(index).start()

            @pl.when(inner)
            def _():
                for kind in range(2):
                    for x in range(2):
                        deep_near_out[index, x, kind] = full[index, kind, rim * 2 + x, bottom].astype(half)
                deep_near_copy(index).start()

    def line(index, kind, z):
        return full[index, kind, z * 2 + side, top] + pair_in[index, kind, z].astype(wide)

    def straight(index):
        return index >= heads - direct

    def direct_copy(index, kind, off):
        n = index - (heads - direct)
        return remote(direct_out.at[n, kind, off - 1], direct_in.at[n, kind, off - 1],
                      line_send, direct_recv.at[n, kind], at((mine + off) % sides))

    def relay(index):
        @pl.when(jnp.logical_not(straight(index)))
        def _():
            pair_copy(index).wait_recv()

            @pl.when(outer)
            def _():
                for kind in range(2):
                    for j in range(sides - 1):
                        edge_out[index, kind, j] = line(index, kind, (rim + 1 + j) % sides).astype(half)
                edge_copy(index).start()

            @pl.when(inner)
            def _():
                for kind in range(2):
                    near_out[index, kind] = line(index, kind, rim).astype(half)
                near_copy(index).start()

            for kind in range(2):
                outs[kind][top, columns(index)] = line(index, kind, mine)

        if direct:
            @pl.when(straight(index))
            def _():
                for kind in (1, 0):
                    last_copy(index, kind).wait_recv()
                    for off in sorted(range(1, sides), key=lambda o: abs(o - sides // 2)):
                        direct_out[index - (heads - direct), kind, off - 1] = (
                            line(index, kind, (mine + off) % sides).astype(half)
                        )
                        direct_copy(index, kind, off).start()
                    outs[kind][top, columns(index)] = line(index, kind, mine)

    mid = (hub - rim - 1 + sides) % sides

    def merge(index):
        @pl.when(jnp.logical_and(inner, jnp.logical_not(straight(index))))
        def _():
            edge_copy(index).wait_recv()
            for off in range(1, pairs):
                for member in range(2):
                    z = ((group + off) % pairs) * 2 + member
                    for kind in range(2):
                        far_out[index, off - 1, member, kind] = (
                            line(index, kind, z) + edge_in[index, kind, (z - rim - 1 + sides) % sides].astype(wide)
                        ).astype(half)
                    far_copy(index, off, member).start()
            for kind in range(2):
                outs[kind][top, columns(index)] += edge_in[index, kind, mid].astype(wide)

        @pl.when(jnp.logical_and(outer, jnp.logical_not(straight(index))))
        def _():
            near_copy(index).wait_recv()
            for kind in range(2):
                outs[kind][top, columns(index)] += near_in[index, kind].astype(wide)

    def gather(index, kind, terms):
        total = outs[kind][top, columns(index)]
        for term in terms:
            total = total + term.astype(wide)
        outs[kind][top, columns(index)] = total

    def finish(index):
        @pl.when(jnp.logical_not(straight(index)))
        def _():
            drain(far_in.at[index], far_recv.at[index])
            for kind in range(2):
                gather(index, kind, [far_in[index, n, kind] for n in range(pairs - 1)])

        if direct:
            @pl.when(straight(index))
            def _():
                n = index - (heads - direct)
                for kind in (1, 0):
                    drain(direct_in.at[n, kind], direct_recv.at[n, kind])
                    gather(index, kind, [direct_in[n, kind, off] for off in range(sides - 1)])

    def deep_merge(index):
        @pl.when(inner)
        def _():
            deep_edge_copy(index).wait_recv()
            for off in range(1, pairs):
                for member in range(2):
                    z = ((group + off) % pairs) * 2 + member
                    for kind in range(2):
                        for x in range(2):
                            deep_far_out[index, off - 1, member, x, kind] = (
                                full[index, kind, z * 2 + x, bottom]
                                + deep_edge_in[index, (z - rim - 1 + sides) % sides, x, kind].astype(wide)
                            ).astype(half)
                    deep_far_copy(index, off, member).start()
            for kind in range(2):
                for x in range(2):
                    full[index, kind, mine * 2 + x, bottom] += deep_edge_in[index, mid, x, kind].astype(wide)

        @pl.when(outer)
        def _():
            deep_near_copy(index).wait_recv()
            for kind in range(2):
                for x in range(2):
                    full[index, kind, mine * 2 + x, bottom] += deep_near_in[index, x, kind].astype(wide)

    def deep_cross(index):
        drain(deep_far_in.at[index], deep_far.at[index])

        def total(kind, x):
            value = full[index, kind, mine * 2 + x, bottom]
            for off in range(1, pairs):
                value = value + deep_far_in[index, off - 1, x, kind].astype(wide)
            return value

        for kind in range(2):
            cross_out[index, kind] = total(kind, other).astype(half)
        cross_copy(index).start()
        for kind in range(2):
            outs[kind][bottom, columns(index)] = total(kind, side)

    def deep_finish(index):
        cross_copy(index).wait_recv()
        for kind in range(2):
            outs[kind][bottom, columns(index)] += cross_in[index, kind].astype(wide)

    def natural(t, run):
        low, high = due(t)

        def one(index, carry):
            run(index)
            return carry

        lax.fori_loop(low, high, one, 0)

    def step(i, carry):
        @pl.when(i < heads)
        def _():
            compute(i)

        @pl.when(i == min(LAGS[1], DEEP_LAGS[0]))
        def _():
            @pl.when(inner)
            def _():
                pl.semaphore_wait(ready, pairs - 1)
                if direct:
                    greet(at(rim), open_line)

            if direct:
                @pl.when(outer)
                def _():
                    pl.semaphore_wait(open_line, 1)

        def after(lag, run):
            if lag is None:
                return

            @pl.when(jnp.logical_and(i >= lag, i < heads + lag))
            def _():
                run(i - lag)

        after(DEEP_LAGS[0] if deep else None, lambda t: natural(t, deep_merge))
        after(DEEP_LAGS[1] if deep else None, lambda t: natural(t, deep_cross))
        after(LAGS[1], lambda t: natural(t, merge))
        after(LAGS[0], lambda t: relay(head_at(t)))
        after(LAGS[2], lambda t: natural(t, finish))
        after(DEEP_LAGS[2] if deep else None, lambda t: natural(t, deep_finish))
        return carry

    last = heads + max(LAGS[2], DEEP_LAGS[2] if deep else 0)
    lax.fori_loop(0, last, step, 0)

    drain(latents.at[:, :, pl.ds(0, owned), :], latent_send)
    drain(latents.at[pl.ds(0, heads - relief), :, far_rows, :], latent_send)
    for ref in (pair_out, cross_out) if deep else (pair_out,):
        drain(ref, pair_send)

    plain = pl.ds(0, heads - direct)
    if direct:
        drain(direct_out, line_send)

    @pl.when(outer)
    def _():
        drain(edge_out.at[plain], line_send)
        if deep:
            drain(deep_edge_out, line_send)

    @pl.when(inner)
    def _():
        if relief:
            drain(latents.at[pl.ds(0, 2 * relief), :, far_rows, :], latent_send)
        for ref in (near_out.at[plain], far_out.at[plain]) + ((deep_near_out, deep_far_out) if deep else ()):
            drain(ref, line_send)


def attention(images_n, texts_n, order, gate, seen, query, grad, key, value):
    tokens, width = query.shape
    heads = gate.shape[1]
    head_width = width // heads
    rows = key.shape[0] * images_n
    sides = texts_n // 2
    pairs = sides // 2
    share = rows // texts_n
    relief = heads // RELIEF if pairs % 2 == 0 and images_n > 2 else 0
    deep = DEEP if DEEP <= share // 8 else 0
    vmem = pl.BlockSpec(memory_space=pltpu.VMEM)
    hbm = pl.BlockSpec(memory_space=pl.ANY)
    half = jnp.bfloat16
    dma = pltpu.SemaphoreType.DMA((heads,))
    two = pltpu.SemaphoreType.DMA((2, 2))
    pair = pltpu.SemaphoreType.DMA((2,))
    single = pltpu.SemaphoreType.DMA(())
    block = (share - deep, head_width)
    direct = DIRECT if sides <= 4 else 0
    last = pltpu.SemaphoreType.DMA((max(direct, 1), 2))
    small = (max(deep, 8), head_width)
    units = (heads, 2)
    return pl.pallas_call(
        functools.partial(kernel, images_n, sides, relief, direct),
        in_specs=[hbm] * 7,
        out_specs=[vmem, vmem, vmem],
        out_shape=[pltpu.VMEM((tokens, width), half)] + [pltpu.VMEM((share, width), jnp.float32)] * 2,
        scratch_shapes=[
            pltpu.SMEM(order.shape, order.dtype), pltpu.VMEM(gate.shape, gate.dtype), pltpu.VMEM(seen.shape, seen.dtype),
            pltpu.VMEM((order.shape[1], tokens), jnp.float32),
            pltpu.VMEM((heads, tokens, head_width), half),
            pltpu.VMEM((heads, tokens, head_width), half),
            pltpu.VMEM((heads, 2, rows, head_width), half),
            pltpu.VMEM((*units, texts_n, share, head_width), jnp.float32),
            pltpu.VMEM((*units, sides, *block), half),
            pltpu.VMEM((*units, sides, *block), half),
            pltpu.VMEM((*units, sides - 1, *block), half),
            pltpu.VMEM((*units, sides - 1, *block), half),
            pltpu.VMEM((*units, *block), half),
            pltpu.VMEM((*units, *block), half),
            pltpu.VMEM((heads, pairs - 1, 2, 2, *block), half),
            pltpu.VMEM((heads, pairs - 1, 2, *block), half),
            pltpu.VMEM((heads, sides - 1, 2, 2, *small), half),
            pltpu.VMEM((heads, sides - 1, 2, 2, *small), half),
            pltpu.VMEM((heads, 2, 2, *small), half),
            pltpu.VMEM((heads, 2, 2, *small), half),
            pltpu.VMEM((heads, pairs - 1, 2, 2, 2, *small), half),
            pltpu.VMEM((heads, pairs - 1, 2, 2, *small), half),
            pltpu.VMEM((*units, *small), half),
            pltpu.VMEM((*units, *small), half),
            pltpu.VMEM((max(direct, 1), 2, sides - 1, *block), half),
            pltpu.VMEM((max(direct, 1), 2, sides - 1, *block), half),
            pltpu.VMEM((images_n - 2, 2, rows // images_n, head_width), half),
            two, pair, dma, single, single, dma, single, dma, last, dma,
            dma, dma, dma, last, pltpu.SemaphoreType.DMA((4,)),
            pltpu.SemaphoreType.REGULAR, pltpu.SemaphoreType.REGULAR,
        ],
        compiler_params=pltpu.CompilerParams(
            vmem_limit_bytes=56 * 1024 * 1024, collective_id=0, has_side_effects=True
        ),
    )(order, gate, seen, query, grad, key, value)


def publish(*arrays):
    def body(*refs):
        count = len(arrays)
        sems = refs[-1]
        copies = [pltpu.make_async_copy(refs[n], refs[count + n], sems.at[n]) for n in range(count)]
        for copy in copies:
            copy.start()
        for copy in copies:
            copy.wait()

    return pl.pallas_call(
        body,
        in_specs=[pl.BlockSpec(memory_space=pltpu.VMEM)] * len(arrays),
        out_specs=[pl.BlockSpec(memory_space=pl.ANY)] * len(arrays),
        out_shape=[jax.ShapeDtypeStruct(array.shape, array.dtype) for array in arrays],
        scratch_shapes=[pltpu.SemaphoreType.DMA((len(arrays),))],
        compiler_params=pltpu.CompilerParams(vmem_limit_bytes=1024 * 1024),
    )(*[pltpu.with_memory_space_constraint(array, pltpu.VMEM) for array in arrays])


def shards(images_n, texts_n, queries, visual_keys, visual_values, out_grad, gate_value, image_order, image_seen):
    query_grad, key_share, value_share = publish(*attention(
        images_n, texts_n, image_order, gate_value, image_seen,
        queries[0], out_grad[0], visual_keys[0], visual_values[0]
    ))
    return (query_grad[None], key_share[None], value_share[None])


def solution(mesh):
    placed = (
        P(None, "txt", "img"),
        P(None, "img", None),
        P(None, "img", None),
        P(None, "txt", "img"),
        P(None, "img"),
        P(),
        P("txt"),
    )
    return jax.shard_map(
        functools.partial(shards, mesh.shape["img"], mesh.shape["txt"]),
        mesh=mesh,
        in_specs=placed,
        out_specs=(P(None, "txt", "img"), P(None, "txt", "img"), P(None, "txt", "img")),
        check_vma=False,
    )
```
